32 devices in a mesh: groups: 1, ctx: 8 (over z, y), head: 2 (over x), rep: 2 (over core).
Axes of the slice: x: 2, y: 2, z: 4, core: 2. Of those that a mesh axis runs over, the one named last changes fastest.
Arguments:
- queries: bfloat16 [16, 512, 4096], P(('groups', 'ctx'), 'rep', 'head'), may hold values from -6 to 6
- prefill_keys: bfloat16 [16, 512, 1024], P(('groups', 'ctx'), 'rep', 'head'), may hold values from -6 to 6
- prefill_values: bfloat16 [16, 512, 1024], P(('groups', 'ctx'), 'rep', 'head'), may hold values from -6 to 6
- context_keys: bfloat16 [16384, 1024], P(('groups', 'ctx'), 'head'), may hold values from -6 to 6
- context_values: bfloat16 [16384, 1024], P(('groups', 'ctx'), 'head'), may hold values from -6 to 6
- picks: int32 [16, 32, 3], P(('groups', 'ctx'), 'head'), may hold values from 0 to 47, as said below
Outputs:
- attended: bfloat16 [16, 512, 4096], P(('groups', 'ctx'), 'rep', 'head')
The draws below stay inside these ranges and needn't reach their ends.
Inputs may be any that keep to these rules, and one draw needn't show every extreme that they name: `picks`: row [b, h] is increasing; its last entry is 32 + b and its first two are cache blocks. Among the first two entries of the rows of the 2 query blocks that start at a multiple of 2 and the 16 heads of one run that starts at a multiple of 16, at most 16 lie in the 4 blocks that start at one multiple of 4, and for every such set of rows some such set of blocks holds exactly 16 of them.
All inputs are finite; a program needn't handle non-finite values.
Results may differ from the reference program's by a relative error of at most 0.0055.
Values may be sent and summed in bfloat16 or wider, within the bound.
A program may use at most 64 MiB of HBM per device.

```python
import jax
import jax.numpy as jnp
from jax import lax

QUERY_HEAD_COUNT = 32
KEY_VALUE_HEADS = 8
HEAD_WIDTH = 128
BLOCK_TOKENS = 512
QB_DEV = 2
BLK_DEV = 4
CACHE_BLOCKS = 32
CACHE_TOKENS = 16384
QUERY_BLOCKS = 16
PREFILL_TOKENS = 8192
CAP = 16
N_CTX = 8
N_HEAD = 2


def key_record_field(key, salt, stack_height):
    array_shape = (stack_height, KEY_VALUE_HEADS, HEAD_WIDTH)
    record_field = jnp.clip(jax.random.normal(jax.random.fold_in(key, salt), array_shape, jnp.float32), -6.0, 6.0)
    return record_field.reshape(stack_height, KEY_VALUE_HEADS * HEAD_WIDTH).astype(jnp.bfloat16)


def draw_queries(key, part):
    array_shape = (PREFILL_TOKENS, QUERY_HEAD_COUNT, HEAD_WIDTH)
    record_field = jnp.clip(jax.random.normal(jax.random.fold_in(key, 11), array_shape, jnp.float32), -6.0, 6.0)
    return record_field.reshape(QUERY_BLOCKS, BLOCK_TOKENS, QUERY_HEAD_COUNT * HEAD_WIDTH).astype(jnp.bfloat16)


def draw_prefill_keys(key, part):
    return key_record_field(key, 21, PREFILL_TOKENS).reshape(QUERY_BLOCKS, BLOCK_TOKENS, KEY_VALUE_HEADS * HEAD_WIDTH)


def draw_context_keys(key, part):
    return key_record_field(key, 31, CACHE_TOKENS)


def draw_picks(key, part):
    head_grouping = QUERY_HEAD_COUNT // N_HEAD
    runs = QB_DEV * head_grouping
    needed = 2 * runs
    slot_total = N_CTX * CAP
    tokens = jnp.arange(slot_total)
    columns = []
    for head_index in range(N_HEAD):
        head_key = jax.random.fold_in(key, 100 + head_index)
        hottest = jax.random.randint(jax.random.fold_in(head_key, 1), (), 0, N_CTX)

        def single(row_key, row_index):
            subkeys = jax.random.split(row_key, 5)
            shuffled = jax.random.permutation(subkeys[0], slot_total)
            ranking = jnp.where(tokens // CAP == hottest, tokens % CAP, CAP + shuffled)
            taken = jnp.argsort(ranking, stable=True)[:needed]
            taken = jax.random.permutation(subkeys[1], taken)
            holders = (taken // CAP).reshape(runs, 2)
            leading = jax.random.randint(subkeys[2], (runs,), 0, BLK_DEV)
            shifted = (leading + 1 + jax.random.randint(subkeys[3], (runs,), 0, BLK_DEV - 1)) % BLK_DEV
            loose = jax.random.randint(subkeys[4], (runs,), 0, BLK_DEV)
            trailing = jnp.where(holders[:, 0] == holders[:, 1], shifted, loose)
            earlier = holders[:, 0] * BLK_DEV + leading
            later = holders[:, 1] * BLK_DEV + trailing
            ownblock = CACHE_BLOCKS + row_index * QB_DEV + jnp.arange(runs, dtype=jnp.int32) // head_grouping
            stacked = jnp.stack([jnp.minimum(earlier, later), jnp.maximum(earlier, later), ownblock], axis=1)
            return stacked.reshape(QB_DEV, head_grouping, 3)
        row_keys = jax.random.split(jax.random.fold_in(head_key, 2), N_CTX)
        columns.append(jax.vmap(single)(row_keys, jnp.arange(N_CTX, dtype=jnp.int32)))
    return jnp.concatenate(columns, axis=2).reshape(QUERY_BLOCKS, QUERY_HEAD_COUNT, 3).astype(jnp.int32)


def block_levels(stream_key, extent, cuts, smallest, largest):
    factor_of, own = 1.0, jax.random.fold_in(stream_key, 6)
    for axis_at, blocks in cuts:
        heights = jnp.exp(jax.random.uniform(jax.random.fold_in(own, axis_at), (blocks,), jnp.float32, smallest / len(cuts), largest / len(cuts)))
        factor_of = factor_of * jnp.repeat(heights, extent[axis_at] // blocks).reshape([-1 if axis == axis_at else 1 for axis in range(len(extent))])
    return factor_of


def normal_values(key, extent, scale, most, shards=(), kind=jnp.bfloat16):
    array = scale * jax.random.normal(key, extent, jnp.float32)
    if shards:
        array = array * block_levels(key, extent, shards, -0.22, 0.18)
    return jnp.clip(array, -most, most).astype(kind)


def setup_inputs(seed: int = 0, part: int = 0) -> dict:
    arg_keys = jax.random.split(jax.random.key(seed), 7)
    part_splits = jax.random.split(jax.random.fold_in(arg_keys[6], part), 7)
    return {
        "queries": draw_queries(jax.random.fold_in(jax.random.fold_in(arg_keys[6], part), 71), part),
        "prefill_keys": draw_prefill_keys(jax.random.fold_in(jax.random.fold_in(arg_keys[6], part), 71), part),
        "prefill_values": normal_values(part_splits[2], (QUERY_BLOCKS, BLOCK_TOKENS, KEY_VALUE_HEADS * HEAD_WIDTH), 1.0, 6.0, ((0, 8), (1, 2), (2, 2))),
        "context_keys": draw_context_keys(jax.random.fold_in(jax.random.fold_in(arg_keys[6], part), 71), part),
        "context_values": normal_values(part_splits[4], (CACHE_TOKENS, KEY_VALUE_HEADS * HEAD_WIDTH), 1.0, 6.0, ((0, 8), (1, 2))),
        "picks": draw_picks(jax.random.fold_in(jax.random.fold_in(arg_keys[6], part), 71), part),
    }


NEGATIVE = -1e30


def partial_attention(scores, values, allowed, pattern):
    scores = jnp.where(allowed, scores, NEGATIVE)
    highest = jnp.max(scores, axis=-1, keepdims=True)
    weights = jnp.exp(scores - highest)
    totals = jnp.sum(weights, axis=-1, keepdims=True)
    rounded = lax.optimization_barrier(weights.astype(jnp.bfloat16)).astype(jnp.float32)
    mixed = jnp.einsum(pattern, rounded, values.astype(jnp.float32))
    return mixed / totals, highest[..., 0] + jnp.log(totals[..., 0])


def reference(queries, prefill_keys, prefill_values, context_keys, context_values, picks):
    head_grouping = QUERY_HEAD_COUNT // KEY_VALUE_HEADS
    scale = HEAD_WIDTH ** -0.5
    owning_head = jnp.arange(QUERY_HEAD_COUNT, dtype=jnp.int32) // head_grouping
    key_tiles = context_keys.reshape(CACHE_BLOCKS, BLOCK_TOKENS, KEY_VALUE_HEADS, HEAD_WIDTH)
    value_tiles = context_values.reshape(CACHE_BLOCKS, BLOCK_TOKENS, KEY_VALUE_HEADS, HEAD_WIDTH)
    places = jnp.arange(BLOCK_TOKENS, dtype=jnp.int32)
    causal = places[None, :] <= places[:, None]

    def one_block(block_index):
        block_queries = lax.dynamic_index_in_dim(queries, block_index, 0, keepdims=False).reshape(BLOCK_TOKENS, QUERY_HEAD_COUNT, HEAD_WIDTH).astype(jnp.float32)
        selected_block_keys = lax.dynamic_index_in_dim(prefill_keys, block_index, 0, keepdims=False).reshape(BLOCK_TOKENS, KEY_VALUE_HEADS, HEAD_WIDTH)[:, owning_head, :].astype(jnp.float32)
        selected_block_values = lax.dynamic_index_in_dim(prefill_values, block_index, 0, keepdims=False).reshape(BLOCK_TOKENS, KEY_VALUE_HEADS, HEAD_WIDTH)[:, owning_head, :].astype(jnp.float32)
        scores = jnp.einsum("rhd,jhd->hrj", block_queries, selected_block_keys) * scale
        own_mixed, own_log = partial_attention(scores, selected_block_values, causal, "hrj,jhd->hrd")
        chosen = lax.dynamic_index_in_dim(picks, block_index, 0, keepdims=False)
        parts = [own_mixed]
        logs = [own_log]
        for column in range(2):
            blocks = chosen[:, column]
            keys_here = key_tiles[blocks, :, owning_head, :].astype(jnp.float32)
            values_here = value_tiles[blocks, :, owning_head, :].astype(jnp.float32)
            scores = jnp.einsum("rhd,hjd->hrj", block_queries, keys_here) * scale
            mixed, logged = partial_attention(scores, values_here, True, "hrj,hjd->hrd")
            mixed = lax.optimization_barrier(mixed.astype(jnp.bfloat16)).astype(jnp.float32)
            parts.append(mixed)
            logs.append(logged)
        all_logs = jnp.stack(logs, 0)
        all_mixed = jnp.stack(parts, 0)
        peak = jnp.max(all_logs, axis=0, keepdims=True)
        shares = jnp.exp(all_logs - peak)
        merged = jnp.sum(shares[..., None] * all_mixed, axis=0) / jnp.sum(shares, axis=0)[..., None]
        return jnp.transpose(merged, (1, 0, 2)).reshape(BLOCK_TOKENS, QUERY_HEAD_COUNT * HEAD_WIDTH).astype(jnp.bfloat16)

    return lax.map(one_block, jnp.arange(QUERY_BLOCKS, dtype=jnp.int32))
```

```python
import functools
import math

import jax
import jax.numpy as jnp
from jax import lax
from jax.experimental import pallas as pl
from jax.experimental.pallas import tpu as pltpu
from jax.sharding import PartitionSpec as P


HEAD_WIDTH = 128
BLOCK_TOKENS = 512


NEGATIVE = -1e30


def from_behind(value, axis, steps):
    count = lax.axis_size(axis)
    first, last = (max(0, -steps), min(count, count - steps))
    return lax.ppermute(value, axis, [(source, source + steps) for source in range(first, last)])


def partial_attention(scores, values, allowed, pattern):
    scores = jnp.where(allowed, scores, NEGATIVE)
    highest = jnp.max(scores, axis=-1, keepdims=True)
    weights = jnp.exp(scores - highest)
    totals = jnp.sum(weights, axis=-1, keepdims=True)
    mixed = jnp.einsum(
        pattern, weights.astype(jnp.bfloat16), values, preferred_element_type=jnp.float32
    )
    return (mixed / totals, highest[..., 0] + jnp.log(totals[..., 0]))


def assign_slots(chosen, blocks_here, capacity):
    flat = chosen.reshape(-1)
    holders = flat // blocks_here
    places = jnp.arange(flat.shape[0])
    earlier = jnp.sum(
        (holders[:, None] == holders[None, :]) & (places[None, :] < places[:, None]), axis=1
    )
    return (holders * capacity + earlier, flat - holders * blocks_here)


def routed_body(queries, prefill_keys, prefill_values, context_keys, context_values, picks):
    local_count = queries.shape[0]
    stack_height = queries.shape[1]
    query_heads = queries.shape[2] // HEAD_WIDTH
    key_heads = prefill_keys.shape[2] // HEAD_WIDTH
    head_grouping = query_heads // key_heads
    blocks_here = context_keys.shape[0] // BLOCK_TOKENS
    ctx_size = lax.axis_size("ctx")
    pick_count = 2 * local_count * query_heads
    capacity = max(2, 2 * pick_count // ctx_size)
    slot_count = ctx_size * capacity
    scale = HEAD_WIDTH ** (-0.5)
    rep_index = lax.axis_index("rep")
    earlier_keys, earlier_values = from_behind((prefill_keys, prefill_values), "rep", 1)
    selected_block_keys = jnp.concatenate([earlier_keys, prefill_keys], 1).reshape(
        local_count, 2 * stack_height, key_heads, HEAD_WIDTH
    )
    selected_block_values = jnp.concatenate([earlier_values, prefill_values], 1).reshape(
        local_count, 2 * stack_height, key_heads, HEAD_WIDTH
    )
    grouped = queries.reshape(local_count, stack_height, key_heads, head_grouping, HEAD_WIDTH)
    query_place = rep_index * stack_height + jnp.arange(stack_height)
    key_place = (rep_index - 1) * stack_height + jnp.arange(2 * stack_height)
    allowed = (key_place[None, :] <= query_place[:, None]) & (key_place[None, :] >= 0)

    def own_block(paired):
        rows_here, keys_here, values_here = paired
        scores = (
            jnp.einsum("rkgd,jkd->kgrj", rows_here, keys_here, preferred_element_type=jnp.float32)
            * scale
        )
        return partial_attention(scores, values_here, allowed, "kgrj,jkd->kgrd")

    own_mixed, own_log = lax.map(own_block, (grouped, selected_block_keys, selected_block_values))
    own_mixed = own_mixed.reshape(local_count, query_heads, stack_height, HEAD_WIDTH)
    own_log = own_log.reshape(local_count, query_heads, stack_height)
    targets, local_blocks = assign_slots(picks[:, :, :2], blocks_here, capacity)
    routing = targets[:, None] == jnp.arange(slot_count)[None, :]
    sending = routing.astype(jnp.bfloat16).reshape(local_count, query_heads, 2, slot_count)
    by_head = queries.reshape(local_count, stack_height, query_heads, HEAD_WIDTH)
    outbound = jnp.einsum("qhps,qrhd->srd", sending, by_head, preferred_element_type=jnp.float32)
    outbound = outbound.astype(jnp.bfloat16).reshape(ctx_size, capacity, stack_height, HEAD_WIDTH)
    pick_heads = jnp.arange(pick_count) // 2 % query_heads // head_grouping
    key_tiles = context_keys.reshape(blocks_here, BLOCK_TOKENS, key_heads, HEAD_WIDTH)
    value_tiles = context_values.reshape(blocks_here, BLOCK_TOKENS, key_heads, HEAD_WIDTH)
    block_label = jnp.sum(jnp.where(routing, local_blocks[:, None], 0), axis=0)
    head_label = jnp.sum(jnp.where(routing, pick_heads[:, None], 0), axis=0)
    labels = jnp.stack([block_label, head_label], axis=-1).reshape(ctx_size, capacity, 2)
    inbound = lax.all_to_all(outbound, "ctx", split_axis=0, concat_axis=0, tiled=True)
    arrived = lax.all_to_all(labels, "ctx", split_axis=0, concat_axis=0, tiled=True)
    leading = inbound.shape[:2]

    def single(paired):
        rows_in, position = paired
        anchor = (position[0], 0, position[1], 0)
        keys_tile = lax.dynamic_slice(key_tiles, anchor, (1, BLOCK_TOKENS, 1, HEAD_WIDTH)).reshape(
            BLOCK_TOKENS, HEAD_WIDTH
        )
        values_tile = lax.dynamic_slice(
            value_tiles, anchor, (1, BLOCK_TOKENS, 1, HEAD_WIDTH)
        ).reshape(BLOCK_TOKENS, HEAD_WIDTH)
        scores = (
            lax.dot_general(
                rows_in, keys_tile, (((1,), (1,)), ((), ())), preferred_element_type=jnp.float32
            )
            * scale
        )
        mixed, logged = partial_attention(scores, values_tile, True, "rj,jd->rd")
        return (mixed.astype(jnp.bfloat16), logged)

    flat_rows = inbound.reshape((-1,) + inbound.shape[2:])
    flat_labels = arrived.reshape(-1, 2)
    mixed, logged = lax.map(single, (flat_rows, flat_labels), batch_size=8)
    served = mixed.reshape(leading + mixed.shape[1:])
    served_logs = logged.reshape(leading + logged.shape[1:])
    answers = lax.all_to_all(served, "ctx", split_axis=0, concat_axis=0, tiled=True)
    answer_logs = lax.all_to_all(served_logs, "ctx", split_axis=0, concat_axis=0, tiled=True)
    gathered = answers.reshape(slot_count, stack_height, HEAD_WIDTH)[targets]
    gathered_logs = answer_logs.reshape(slot_count, stack_height)[targets]
    remote_mixed = gathered.astype(jnp.float32).reshape(
        local_count, query_heads, 2, stack_height, HEAD_WIDTH
    )
    remote_logs = gathered_logs.reshape(local_count, query_heads, 2, stack_height)
    all_logs = jnp.concatenate([own_log[:, :, None], remote_logs], axis=2)
    all_mixed = jnp.concatenate([own_mixed[:, :, None], remote_mixed], axis=2)
    peak = jnp.max(all_logs, axis=2, keepdims=True)
    shares = jnp.exp(all_logs - peak)
    merged = jnp.sum(shares[..., None] * all_mixed, axis=2) / jnp.sum(shares, axis=2)[..., None]
    return (
        jnp.transpose(merged, (0, 2, 1, 3))
        .reshape(local_count, stack_height, query_heads * HEAD_WIDTH)
        .astype(jnp.bfloat16)
    )


RATE = HEAD_WIDTH ** (-0.5) * math.log2(math.e)
MESH = pl.DeviceIdType.MESH
LINE = 4
ROWS = BLOCK_TOKENS // 2
PHASES = 4
CHUNKS = 2 * LINE


def score(rows, keys):
    return lax.dot_general(
        rows, keys, (((1,), (1,)), ((), ())), preferred_element_type=jnp.float32
    )


def fold(parts, values, peak, total, mixed):
    highest = jnp.max(parts[0], axis=-1, keepdims=True)
    for part in parts[1:]:
        highest = jnp.maximum(highest, jnp.max(part, axis=-1, keepdims=True))
    if peak is not None:
        highest = jnp.maximum(peak, highest)
        fade = jnp.exp2((peak - highest) * RATE)
        total = total * fade
        mixed = mixed * fade
    for part, value in zip(parts, values):
        weights = jnp.exp2((part - highest) * RATE)
        added = jnp.sum(weights, axis=-1, keepdims=True)
        product = jnp.dot(weights.astype(jnp.bfloat16), value, preferred_element_type=jnp.float32)
        total = added if total is None else total + added
        mixed = product if mixed is None else mixed + product
    return highest, total, mixed


def pack(peak, total):
    lane = lax.broadcasted_iota(jnp.int32, (peak.shape[0], HEAD_WIDTH), 1)
    return jnp.where(lane < HEAD_WIDTH // 2, peak, total)


def unpack(packed):
    return packed[:, :1], packed[:, HEAD_WIDTH // 2 : HEAD_WIDTH // 2 + 1]


def aligned(index, width):
    return pl.ds(pl.multiple_of(index * width, width), width)


def span_kernel(
    table_in,
    q_in,
    pk_in,
    pv_in,
    ck_in,
    cv_in,
    out,
    kv0,
    kv1,
    kv2,
    kv3,
    qs,
    own,
    table,
    picked,
    acc,
    stat,
    ans,
    ahead_sem,
    back_sem,
    twin_sem,
    link_sem,
    twin_recv,
    side_sem,
    load_sem,
    q_send,
    q_recv,
    own_send,
    own_recv,
    table_send,
    table_recv,
    picked_sem,
    ans_send,
    ans_recv,
):
    kv = (kv0, kv1, kv2, kv3)
    me, r = lax.axis_index("ctx"), lax.axis_index("rep")
    z, y = me // 2, me % 2
    side = z // 2
    inner = (z + side) % 2
    z_twin = z + 1 - 2 * (z % 2)
    z_ahead = inner * (3 - z) + (1 - inner) * z_twin
    is_inner, is_outer = inner == 1, inner == 0
    query_heads = q_in.shape[2] // HEAD_WIDTH
    group = query_heads // (pk_in.shape[2] // HEAD_WIDTH)
    width = group * HEAD_WIDTH
    pairs = group // 2
    blocks_here = ck_in.shape[0]
    half = blocks_here // 2
    count = q_in.shape[0]

    def remote(src, dst, send, recv, ctx, rep):
        return pltpu.make_async_remote_copy(
            src_ref=src,
            dst_ref=dst,
            send_sem=send,
            recv_sem=recv,
            device_id={"ctx": ctx, "rep": rep},
            device_id_type=MESH,
        )

    def chunk_at(j):
        jj = j // 2
        m = jj + inner * (1 - 2 * jj) * (1 - jj // 2)
        return (m + side * (3 - 2 * m)) * 2 + (y + j % 2) % 2

    def lane(p, ctx, rep):
        return kv[p].at[pl.ds(ctx * blocks_here + rep * half, half)]

    barrier = pltpu.get_barrier_semaphore()

    def greet(ctx, rep):
        pl.semaphore_signal(barrier, inc=1, device_id={"ctx": ctx, "rep": rep}, device_id_type=MESH)

    beside = z * 2 + 1 - y
    greet(me, 1 - r)
    for rep in range(2):
        greet(beside, rep)
        greet(z_twin * 2 + y, rep)
        greet(z_twin * 2 + 1 - y, rep)

    loads = []
    for p in range(PHASES):
        cols = aligned(2 * y + p // 2, HEAD_WIDTH)
        for kind, source in enumerate((ck_in, cv_in)):
            loads.append(
                pltpu.make_async_copy(
                    source.at[:, p % 2, :, cols],
                    kv[p].at[pl.ds(me * blocks_here, blocks_here), kind],
                    load_sem.at[p, kind],
                )
            )
    for load in loads:
        load.start()

    @pl.when(is_inner)
    def _():
        greet((3 - z) * 2 + y, r)
        pl.semaphore_wait(barrier, 8)

    @pl.when(is_outer)
    def _():
        pl.semaphore_wait(barrier, 7)

    def side_copies(p):
        cols = aligned(2 * (1 - y) + p // 2, HEAD_WIDTH)
        return [
            remote(
                source.at[pl.ds(r * half, half), p % 2, :, cols],
                kv[p].at[pl.ds(me * blocks_here + r * half, half), kind],
                side_sem.at[p, kind],
                link_sem.at[p, me],
                beside,
                r,
            )
            for kind, source in enumerate((ck_in, cv_in))
        ]

    def q_copy(late, other, ctx, slot):
        head = 2 * (1 - y if other else y) + late
        place = 4 * late + slot
        src = q_in.at[:, :, aligned(head, width)]
        send = q_send.at[2 * late + other]
        return src, qs.at[place], send, q_recv.at[place]

    def own_copy(late, other, slot, kind, rep):
        head = 2 * (1 - y if other else y) + late
        place = 4 * late + slot
        src = (pk_in, pv_in)[kind].at[:, :, aligned(head, HEAD_WIDTH)]
        send = own_send.at[4 * late + 2 * other + kind, rep]
        return src, own.at[place, kind, r], send, own_recv.at[place, kind, r]

    def feeds():
        todo = []

        def add(cond, late, other, ctx, slot, near):
            src, dst, send, recv = q_copy(late, other, ctx, slot)
            if near:
                todo.append((cond, pltpu.make_async_copy(src, dst, recv), True, (late, other)))
            else:
                todo.append((cond, remote(src, dst, send, recv, ctx, r), False, (late, other)))
            for kind in range(2):
                src, dst, send, recv = own_copy(late, other, slot, kind, 0)
                if near:
                    todo.append((cond, pltpu.make_async_copy(src, dst, recv), True, (late, other)))
                else:
                    todo.append((cond, remote(src, dst, send, recv, ctx, r), False, (late, other)))
                src, dst, send, recv = own_copy(late, other, slot, kind, 1)
                both = r == 0 if cond is None else cond & (r == 0)
                todo.append((both, remote(src, dst, send, recv, ctx, 1), False, (late, other)))

        add(is_inner, 0, 0, me, 0, True)
        add(is_inner, 0, 1, beside, 1, False)
        add(is_outer, 0, 0, z_twin * 2 + y, 2, False)
        add(is_outer, 0, 1, z_twin * 2 + 1 - y, 3, False)
        add(None, 1, 0, me, 0, True)
        add(None, 1, 1, beside, 1, False)
        return todo

    def table_copies():
        return [
            (None, remote(table_in, table.at[1], table_send.at[0], table_recv.at[1], beside, r)),
            (
                is_outer,
                remote(
                    table_in, table.at[2], table_send.at[1], table_recv.at[2], z_twin * 2 + y, r
                ),
            ),
            (
                is_outer,
                remote(
                    table_in, table.at[3], table_send.at[2], table_recv.at[3], z_twin * 2 + 1 - y, r
                ),
            ),
        ]

    def guarded(cond, action):
        if cond is None:
            action()
        else:
            pl.when(cond)(action)

    def ahead_copy(p, j):
        ctx = chunk_at(j)
        return remote(
            lane(p, ctx, r), lane(p, ctx, r), ahead_sem.at[p, j], link_sem.at[p, ctx],
            z_ahead * 2 + y, r,
        )

    def back_copy(p, j):
        ctx = chunk_at(j)
        return remote(
            lane(p, ctx, r), lane(p, ctx, r), back_sem.at[p, j], link_sem.at[p, ctx],
            z_twin * 2 + y, r,
        )

    def twin_copy(p, j):
        ctx = chunk_at(j)
        return remote(
            lane(p, ctx, r), lane(p, ctx, r), twin_sem.at[p, j], twin_recv.at[p, ctx], me, 1 - r
        )

    def sends(p, j):
        late = p >= 2
        out_list = [(j < 2 + 2 * inner, ahead_copy(p, j))]
        if late:
            out_list.append((is_inner & ((j < 2) | (j >= 4)), back_copy(p, j)))
        return out_list

    def relay(p, j):
        ctx = chunk_at(j)
        remote(
            lane(p, ctx, r), lane(p, ctx, r), twin_sem.at[p, j], link_sem.at[p, ctx], me, 1 - r
        ).wait_recv()
        for cond, copy in sends(p, j):
            guarded(cond, copy.start)
        guarded(None if p >= 2 else is_inner, twin_copy(p, j).start)

    def launch(p):
        loads[2 * p].wait()
        loads[2 * p + 1].wait()
        for cond, copy in sends(p, 0):
            guarded(cond, copy.start)

    def complete(p):
        def one(j, carry):
            ctx = chunk_at(j)
            remote(
                lane(p, ctx, 1 - r), lane(p, ctx, 1 - r), twin_sem.at[p, j], twin_recv.at[p, ctx],
                me, 1 - r,
            ).wait_recv()
            return carry

        lax.fori_loop(1, CHUNKS, one, 0)

    todo = feeds()

    def feed(late, other):
        for item in todo:
            if not item[2] and item[3] == (late, other):
                guarded(item[0], item[1].start)

    for item in todo:
        if item[2]:
            guarded(item[0], item[1].start)
    for copy in side_copies(0):
        copy.start()
    for cond, copy in table_copies():
        guarded(cond, copy.start)
    launch(0)

    @pl.when(is_inner)
    def _():
        feed(0, 0)
        feed(0, 1)

    for copy in side_copies(1) + side_copies(2):
        copy.start()
    feed(1, 0)
    feed(1, 1)
    for copy in side_copies(3):
        copy.start()

    def await_slot(place):
        pltpu.make_async_copy(qs.at[place], qs.at[place], q_recv.at[place]).wait()
        for kind in range(2):
            ref = own.at[place, kind, r]
            pltpu.make_async_copy(ref, ref, own_recv.at[place, kind, r]).wait()

        @pl.when(r == 1)
        def _():
            for kind in range(2):
                ref = own.at[place, kind, 0]
                pltpu.make_async_copy(ref, ref, own_recv.at[place, kind, 0]).wait()

    per_slot = count * pairs

    def query(t, u):
        place, b, g = t // per_slot, t % per_slot // pairs, t % pairs
        return qs[place, b, :, aligned(g * 2 + u, HEAD_WIDTH)]

    def own_unit(t):
        place, b = t // per_slot, t % per_slot // pairs
        row = lax.broadcasted_iota(jnp.int32, (ROWS, ROWS), 0)
        column = lax.broadcasted_iota(jnp.int32, (ROWS, ROWS), 1)
        for u in range(2):
            scores = score(query(t, u), own[place, 0, r, b])
            scores = jnp.where(column <= row, scores, NEGATIVE)
            peak, total, mixed = fold([scores], [own[place, 1, r, b]], None, None, None)
            acc[t, u] = mixed
            stat[t, u] = pack(peak, total)

        @pl.when(r == 1)
        def _():
            for u in range(2):
                peak, total = unpack(stat[t, u])
                scores = score(query(t, u), own[place, 0, 0, b])
                peak, total, mixed = fold(
                    [scores], [own[place, 1, 0, b]], peak, total, acc[t, u]
                )
                acc[t, u] = mixed
                stat[t, u] = pack(peak, total)

    def pick_unit(p, t, last):
        place, b, g = t // per_slot, t % per_slot // pairs, t % pairs
        late = p // 2
        slot = place - 4 * late
        head = (2 * y + late) * group + g * 2
        for u in range(2):
            at = (b * query_heads + head + u) * 2
            first = picked[slot, 0, at]
            second = picked[slot, 0, at + 1]
            rows = query(t, u)
            peak, total = unpack(stat[t, u])
            peak, total, mixed = fold(
                [score(rows, kv[p][first, 0]), score(rows, kv[p][second, 0])],
                [kv[p][first, 1], kv[p][second, 1]],
                peak,
                total,
                acc[t, u],
            )
            if last:
                ans[t, :, u * HEAD_WIDTH : (u + 1) * HEAD_WIDTH] = (mixed / total).astype(ans.dtype)
            else:
                acc[t, u] = mixed
                stat[t, u] = pack(peak, total)

    def slab(b, head, g):
        return (head * count + b) * pairs + g

    def answer(t, late, act_near, act_far):
        place, b, g = t // per_slot, t % per_slot // pairs, t % pairs
        slot = place - 4 * late
        head = 2 * y + late
        target = out.at[b, :, aligned(head * pairs + g, 2 * HEAD_WIDTH)]
        zt = z + (slot // 2) * (z_twin - z)
        ctx = zt * 2 + (y + slot % 2) % 2
        near = slot == 0

        @pl.when(near)
        def _():
            act_near(pltpu.make_async_copy(ans.at[t], target, ans_send.at[t]))

        @pl.when(slot > 0)
        def _():
            act_far(
                remote(ans.at[t], target, ans_send.at[t], ans_recv.at[slab(b, head, g)], ctx, r)
            )

    def send_answer(t, late):
        answer(t, late, lambda c: c.start(), lambda c: c.start())

    def stage(first, units, unit, relays, after=None):
        start, stop, phase = relays
        total = stop - start

        def one(i, carry):
            unit(first + i)
            if after is not None:

                @pl.when(i > 0)
                def _():
                    after(first + i - 1)

            if total > 0:
                step = max(1, units // total)

                @pl.when((i % step == step - 1) & (i // step < total))
                def _():
                    relay(phase, start + i // step)

            return carry

        lax.fori_loop(0, units, one, 0)
        if after is not None:
            after(first + units - 1)

        def rest(j, carry):
            relay(phase, j)
            return carry

        done = min(total, units // max(1, units // total)) if total > 0 else 0
        if done < total:
            lax.fori_loop(start + done, stop, rest, 0)

    late_base = 4 * per_slot
    none = (0, 0, 0)

    def own_slot(place, relays):
        await_slot(place)
        stage(place * per_slot, per_slot, own_unit, relays)

    def picks(p, slot, slots, relays):
        late, last = p // 2, p % 2 == 1
        stage(
            (4 * late + slot) * per_slot,
            slots * per_slot,
            functools.partial(pick_unit, p, last=last),
            relays,
            functools.partial(send_answer, late=late) if last else None,
        )

    pltpu.make_async_copy(table_in, table.at[0], table_recv.at[0]).start()

    def await_table(slots):
        for slot in range(slots):
            pltpu.make_async_copy(table.at[slot], table.at[slot], table_recv.at[slot]).wait()
        copy = pltpu.make_async_copy(
            table.at[pl.ds(0, slots)], picked.at[pl.ds(0, slots)], picked_sem.at[0]
        )
        copy.start()
        copy.wait()

    @pl.when(is_inner)
    def _():
        own_slot(0, (1, 4, 0))
        launch(1)
        own_slot(4, (4, 6, 0))
        own_slot(1, (6, CHUNKS, 0))
        launch(2)
        await_table(4)
        complete(0)
        picks(0, 0, 2, (1, 4, 1))
        own_slot(2, (4, 6, 1))
        picks(0, 2, 1, (6, CHUNKS, 1))
        launch(3)
        complete(1)
        picks(1, 0, 3, (1, 4, 2))
        own_slot(3, (4, 6, 2))
        picks(0, 3, 1, (6, CHUNKS, 2))
        picks(1, 3, 1, none)
        own_slot(5, (1, 2, 3))

    @pl.when(is_outer)
    def _():
        own_slot(4, (1, 2, 0))
        feed(0, 0)
        launch(1)
        relay(1, 1)
        feed(0, 1)
        launch(2)
        launch(3)
        await_table(2)
        own_slot(5, (1, 2, 2))
        relay(3, 1)
        lax.fori_loop(2, CHUNKS, lambda j, c: (relay(2, j), c)[1], 0)

    complete(2)
    picks(2, 0, 2, (2, CHUNKS, 3))
    complete(3)
    picks(3, 0, 2, none)

    for item in todo:
        if not item[2]:
            guarded(item[0], item[1].wait_send)
    for cond, copy in table_copies():
        guarded(cond, copy.wait_send)
    for p in range(PHASES):
        for copy in side_copies(p):
            copy.wait_send()

        def drain(j, carry):
            for cond, copy in sends(p, j):
                guarded(cond, copy.wait_send)
            twin = j >= 1 if p >= 2 else (j >= 1) & is_inner
            guarded(twin, twin_copy(p, j).wait_send)
            return carry

        lax.fori_loop(0, CHUNKS, drain, 0)

    def settle(t, late):
        answer(t, late, lambda c: c.wait(), lambda c: c.wait_send())

    @pl.when(is_inner)
    def _():
        lax.fori_loop(0, 4 * per_slot, lambda t, c: (settle(t, 0), c)[1], 0)

    lax.fori_loop(late_base, late_base + 2 * per_slot, lambda t, c: (settle(t, 1), c)[1], 0)

    def landed(k, carry):
        head, b, g = k // per_slot, k % per_slot // pairs, k % pairs
        target = out.at[b, :, aligned(head * pairs + g, 2 * HEAD_WIDTH)]
        near = (head // 2 == y) & ((head % 2 == 1) | is_inner)

        @pl.when(jnp.logical_not(near))
        def _():
            remote(target, target, ans_send.at[0], ans_recv.at[k], me, 1 - r).wait_recv()

        return carry

    lax.fori_loop(0, 4 * per_slot, landed, 0)


def spread_body(queries, prefill_keys, prefill_values, context_keys, context_values, picks):
    count, height, full = queries.shape
    key_heads = prefill_keys.shape[2] // HEAD_WIDTH
    group = full // prefill_keys.shape[2]
    blocks_here = context_keys.shape[0] // BLOCK_TOKENS
    blocks = blocks_here * CHUNKS
    units = 6 * count * group // 2
    lanes = 2 * count * picks.shape[1]
    flat = picks[:, :, :2].reshape(1, lanes).astype(jnp.int32)
    table = jnp.pad(flat, ((0, 7), (0, -lanes % HEAD_WIDTH)))
    split = (blocks_here, 2, ROWS, context_keys.shape[1])
    dma = pltpu.SemaphoreType.DMA
    anywhere = pl.BlockSpec(memory_space=pl.ANY)
    work = (2 * LINE + 4 * 4) * count * group * key_heads // 4
    return pl.pallas_call(
        span_kernel,
        out_shape=jax.ShapeDtypeStruct(queries.shape, queries.dtype),
        in_specs=[anywhere] * 6,
        out_specs=anywhere,
        scratch_shapes=[pltpu.VMEM((blocks, 2, ROWS, HEAD_WIDTH), jnp.bfloat16)] * PHASES
        + [
            pltpu.VMEM((6, count, height, group * HEAD_WIDTH), jnp.bfloat16),
            pltpu.VMEM((6, 2, 2, count, height, HEAD_WIDTH), jnp.bfloat16),
            pltpu.VMEM((4,) + table.shape, jnp.int32),
            pltpu.SMEM((4,) + table.shape, jnp.int32),
            pltpu.VMEM((units, 2, height, HEAD_WIDTH), jnp.float32),
            pltpu.VMEM((units, 2, height, HEAD_WIDTH), jnp.float32),
            pltpu.VMEM((units, height, 2 * HEAD_WIDTH), jnp.bfloat16),
            dma((PHASES, CHUNKS)),
            dma((PHASES, CHUNKS)),
            dma((PHASES, CHUNKS)),
            dma((PHASES, CHUNKS)),
            dma((PHASES, CHUNKS)),
            dma((PHASES, 2)),
            dma((PHASES, 2)),
            dma((4,)),
            dma((6,)),
            dma((8, 2)),
            dma((6, 2, 2)),
            dma((3,)),
            dma((4,)),
            dma((1,)),
            dma((units,)),
            dma((4 * count * group // 2,)),
        ],
        compiler_params=pltpu.CompilerParams(
            collective_id=0, has_side_effects=True, vmem_limit_bytes=60 * 2**20
        ),
        cost_estimate=pl.CostEstimate(
            flops=work * 4 * ROWS * BLOCK_TOKENS * HEAD_WIDTH,
            transcendentals=work * ROWS * BLOCK_TOKENS,
            bytes_accessed=24 * 2**20,
        ),
        name="spread_attend",
    )(
        table,
        queries,
        prefill_keys,
        prefill_values,
        context_keys.reshape(split),
        context_values.reshape(split),
    )


def body(*args):
    queries, prefill_keys, _, context_keys, _, _ = args
    key_heads = prefill_keys.shape[2] // HEAD_WIDTH
    fits = lax.axis_size("ctx") == CHUNKS and lax.axis_size("rep") == 2 and key_heads == 4
    fits = fits and queries.shape[1] == ROWS and context_keys.shape[0] % (2 * BLOCK_TOKENS) == 0
    if fits and queries.shape[2] // prefill_keys.shape[2] % 2 == 0:
        return spread_body(*args)
    return routed_body(*args)


def solution(mesh):
    return jax.shard_map(
        body,
        mesh=mesh,
        in_specs=(
            P(("groups", "ctx"), "rep", "head"),
            P(("groups", "ctx"), "rep", "head"),
            P(("groups", "ctx"), "rep", "head"),
            P(("groups", "ctx"), "head"),
            P(("groups", "ctx"), "head"),
            P(("groups", "ctx"), "head", None),
        ),
        out_specs=P(("groups", "ctx"), "rep", "head"),
        check_vma=False,
    )
```

```python
import functools
import math

import jax
import jax.numpy as jnp
from jax import lax
from jax.experimental import pallas as pl
from jax.experimental.pallas import tpu as pltpu
from jax.sharding import PartitionSpec as P


HEAD_WIDTH = 128
BLOCK_TOKENS = 512


NEGATIVE = -1e30


def from_behind(value, axis, steps):
    count = lax.axis_size(axis)
    first, last = (max(0, -steps), min(count, count - steps))
    return lax.ppermute(value, axis, [(source, source + steps) for source in range(first, last)])


def partial_attention(scores, values, allowed, pattern):
    scores = jnp.where(allowed, scores, NEGATIVE)
    highest = jnp.max(scores, axis=-1, keepdims=True)
    weights = jnp.exp(scores - highest)
    totals = jnp.sum(weights, axis=-1, keepdims=True)
    mixed = jnp.einsum(
        pattern, weights.astype(jnp.bfloat16), values, preferred_element_type=jnp.float32
    )
    return (mixed / totals, highest[..., 0] + jnp.log(totals[..., 0]))


def assign_slots(chosen, blocks_here, capacity):
    flat = chosen.reshape(-1)
    holders = flat // blocks_here
    places = jnp.arange(flat.shape[0])
    earlier = jnp.sum(
        (holders[:, None] == holders[None, :]) & (places[None, :] < places[:, None]), axis=1
    )
    return (holders * capacity + earlier, flat - holders * blocks_here)


def routed_body(queries, prefill_keys, prefill_values, context_keys, context_values, picks):
    local_count = queries.shape[0]
    stack_height = queries.shape[1]
    query_heads = queries.shape[2] // HEAD_WIDTH
    key_heads = prefill_keys.shape[2] // HEAD_WIDTH
    head_grouping = query_heads // key_heads
    blocks_here = context_keys.shape[0] // BLOCK_TOKENS
    ctx_size = lax.axis_size("ctx")
    pick_count = 2 * local_count * query_heads
    capacity = max(2, 2 * pick_count // ctx_size)
    slot_count = ctx_size * capacity
    scale = HEAD_WIDTH ** (-0.5)
    rep_index = lax.axis_index("rep")
    earlier_keys, earlier_values = from_behind((prefill_keys, prefill_values), "rep", 1)
    selected_block_keys = jnp.concatenate([earlier_keys, prefill_keys], 1).reshape(
        local_count, 2 * stack_height, key_heads, HEAD_WIDTH
    )
    selected_block_values = jnp.concatenate([earlier_values, prefill_values], 1).reshape(
        local_count, 2 * stack_height, key_heads, HEAD_WIDTH
    )
    grouped = queries.reshape(local_count, stack_height, key_heads, head_grouping, HEAD_WIDTH)
    query_place = rep_index * stack_height + jnp.arange(stack_height)
    key_place = (rep_index - 1) * stack_height + jnp.arange(2 * stack_height)
    allowed = (key_place[None, :] <= query_place[:, None]) & (key_place[None, :] >= 0)

    def own_block(paired):
        rows_here, keys_here, values_here = paired
        scores = (
            jnp.einsum("rkgd,jkd->kgrj", rows_here, keys_here, preferred_element_type=jnp.float32)
            * scale
        )
        return partial_attention(scores, values_here, allowed, "kgrj,jkd->kgrd")

    own_mixed, own_log = lax.map(own_block, (grouped, selected_block_keys, selected_block_values))
    own_mixed = own_mixed.reshape(local_count, query_heads, stack_height, HEAD_WIDTH)
    own_log = own_log.reshape(local_count, query_heads, stack_height)
    targets, local_blocks = assign_slots(picks[:, :, :2], blocks_here, capacity)
    routing = targets[:, None] == jnp.arange(slot_count)[None, :]
    sending = routing.astype(jnp.bfloat16).reshape(local_count, query_heads, 2, slot_count)
    by_head = queries.reshape(local_count, stack_height, query_heads, HEAD_WIDTH)
    outbound = jnp.einsum("qhps,qrhd->srd", sending, by_head, preferred_element_type=jnp.float32)
    outbound = outbound.astype(jnp.bfloat16).reshape(ctx_size, capacity, stack_height, HEAD_WIDTH)
    pick_heads = jnp.arange(pick_count) // 2 % query_heads // head_grouping
    key_tiles = context_keys.reshape(blocks_here, BLOCK_TOKENS, key_heads, HEAD_WIDTH)
    value_tiles = context_values.reshape(blocks_here, BLOCK_TOKENS, key_heads, HEAD_WIDTH)
    block_label = jnp.sum(jnp.where(routing, local_blocks[:, None], 0), axis=0)
    head_label = jnp.sum(jnp.where(routing, pick_heads[:, None], 0), axis=0)
    labels = jnp.stack([block_label, head_label], axis=-1).reshape(ctx_size, capacity, 2)
    inbound = lax.all_to_all(outbound, "ctx", split_axis=0, concat_axis=0, tiled=True)
    arrived = lax.all_to_all(labels, "ctx", split_axis=0, concat_axis=0, tiled=True)
    leading = inbound.shape[:2]

    def single(paired):
        rows_in, position = paired
        anchor = (position[0], 0, position[1], 0)
        keys_tile = lax.dynamic_slice(key_tiles, anchor, (1, BLOCK_TOKENS, 1, HEAD_WIDTH)).reshape(
            BLOCK_TOKENS, HEAD_WIDTH
        )
        values_tile = lax.dynamic_slice(
            value_tiles, anchor, (1, BLOCK_TOKENS, 1, HEAD_WIDTH)
        ).reshape(BLOCK_TOKENS, HEAD_WIDTH)
        scores = (
            lax.dot_general(
                rows_in, keys_tile, (((1,), (1,)), ((), ())), preferred_element_type=jnp.float32
            )
            * scale
        )
        mixed, logged = partial_attention(scores, values_tile, True, "rj,jd->rd")
        return (mixed.astype(jnp.bfloat16), logged)

    flat_rows = inbound.reshape((-1,) + inbound.shape[2:])
    flat_labels = arrived.reshape(-1, 2)
    mixed, logged = lax.map(single, (flat_rows, flat_labels), batch_size=8)
    served = mixed.reshape(leading + mixed.shape[1:])
    served_logs = logged.reshape(leading + logged.shape[1:])
    answers = lax.all_to_all(served, "ctx", split_axis=0, concat_axis=0, tiled=True)
    answer_logs = lax.all_to_all(served_logs, "ctx", split_axis=0, concat_axis=0, tiled=True)
    gathered = answers.reshape(slot_count, stack_height, HEAD_WIDTH)[targets]
    gathered_logs = answer_logs.reshape(slot_count, stack_height)[targets]
    remote_mixed = gathered.astype(jnp.float32).reshape(
        local_count, query_heads, 2, stack_height, HEAD_WIDTH
    )
    remote_logs = gathered_logs.reshape(local_count, query_heads, 2, stack_height)
    all_logs = jnp.concatenate([own_log[:, :, None], remote_logs], axis=2)
    all_mixed = jnp.concatenate([own_mixed[:, :, None], remote_mixed], axis=2)
    peak = jnp.max(all_logs, axis=2, keepdims=True)
    shares = jnp.exp(all_logs - peak)
    merged = jnp.sum(shares[..., None] * all_mixed, axis=2) / jnp.sum(shares, axis=2)[..., None]
    return (
        jnp.transpose(merged, (0, 2, 1, 3))
        .reshape(local_count, stack_height, query_heads * HEAD_WIDTH)
        .astype(jnp.bfloat16)
    )


RATE = HEAD_WIDTH ** (-0.5) * math.log2(math.e)
MESH = pl.DeviceIdType.MESH
LINE = 4
ROWS = BLOCK_TOKENS // 2
PHASES = 4
CHUNKS = 2 * LINE


def score(rows, keys):
    return lax.dot_general(
        rows, keys, (((1,), (1,)), ((), ())), preferred_element_type=jnp.float32
    )


def fold(parts, values, peak, mixed):
    highest = None
    for part in parts:
        for at in range(0, part.shape[1], HEAD_WIDTH):
            piece = part[:, at : at + HEAD_WIDTH]
            highest = piece if highest is None else jnp.maximum(highest, piece)
    highest = jnp.max(highest, axis=-1, keepdims=True)
    highest = jnp.broadcast_to(highest, (parts[0].shape[0], HEAD_WIDTH))
    if peak is not None:
        highest = jnp.maximum(peak, highest)
        fade = jnp.exp2((peak - highest) * RATE)
        mixed = mixed * jnp.concatenate([fade, fade], axis=1)
    level = highest * RATE
    for part, value in zip(parts, values):
        base = jnp.concatenate([level] * (part.shape[1] // HEAD_WIDTH), axis=1)
        weights = jnp.exp2(part * RATE - base).astype(jnp.bfloat16)
        beside = jnp.concatenate([value, jnp.ones_like(value)], axis=1)
        product = jnp.dot(weights, beside, preferred_element_type=jnp.float32)
        mixed = product if mixed is None else mixed + product
    return highest, mixed


def aligned(index, width):
    return pl.ds(pl.multiple_of(index * width, width), width)


def span_kernel(
    table_in,
    q_in,
    pk_in,
    pv_in,
    ck_in,
    cv_in,
    out,
    kv0,
    kv1,
    kv2,
    kv3,
    qs,
    own,
    table,
    picked,
    acc,
    stat,
    ans,
    ahead_sem,
    back_sem,
    twin_sem,
    link_sem,
    twin_recv,
    side_sem,
    load_sem,
    q_send,
    q_recv,
    own_send,
    pass_send,
    own_recv,
    table_send,
    table_recv,
    picked_sem,
    ans_send,
    ans_recv,
):
    kv = (kv0, kv1, kv2, kv3)
    me, r = lax.axis_index("ctx"), lax.axis_index("rep")
    z, y = me // 2, me % 2
    side = z // 2
    inner = (z + side) % 2
    z_twin = z + 1 - 2 * (z % 2)
    z_ahead = inner * (3 - z) + (1 - inner) * z_twin
    is_inner, is_outer = inner == 1, inner == 0
    query_heads = q_in.shape[2] // HEAD_WIDTH
    group = query_heads // (pk_in.shape[2] // HEAD_WIDTH)
    width = group * HEAD_WIDTH
    blocks_here = ck_in.shape[0]
    half = blocks_here // 2
    count = q_in.shape[0]

    def remote(src, dst, send, recv, ctx, rep):
        return pltpu.make_async_remote_copy(
            src_ref=src,
            dst_ref=dst,
            send_sem=send,
            recv_sem=recv,
            device_id={"ctx": ctx, "rep": rep},
            device_id_type=MESH,
        )

    def chunk_at(j):
        jj = j // 2
        m = jj + inner * (1 - 2 * jj) * (1 - jj // 2)
        return (m + side * (3 - 2 * m)) * 2 + (y + j % 2) % 2

    def lane(p, ctx, rep):
        return kv[p].at[pl.ds(ctx * blocks_here + rep * half, half)]

    barrier = pltpu.get_barrier_semaphore()

    def greet(ctx, rep):
        pl.semaphore_signal(barrier, inc=1, device_id={"ctx": ctx, "rep": rep}, device_id_type=MESH)

    beside = z * 2 + 1 - y
    greet(me, 1 - r)
    greet(beside, r)
    greet(z_twin * 2 + y, r)
    greet(z_twin * 2 + 1 - y, r)

    loads = []
    for p in range(PHASES):
        cols = aligned(2 * y + p // 2, HEAD_WIDTH)
        for kind, source in enumerate((ck_in, cv_in)):
            loads.append(
                pltpu.make_async_copy(
                    source.at[:, p % 2, :, cols],
                    kv[p].at[pl.ds(me * blocks_here, blocks_here), kind],
                    load_sem.at[p, kind],
                )
            )
    for load in loads:
        load.start()

    @pl.when(is_inner)
    def _():
        greet((3 - z) * 2 + y, r)
        pl.semaphore_wait(barrier, 5)

    @pl.when(is_outer)
    def _():
        pl.semaphore_wait(barrier, 4)

    def side_copies(p):
        cols = aligned(2 * (1 - y) + p // 2, HEAD_WIDTH)
        return [
            remote(
                source.at[pl.ds(r * half, half), p % 2, :, cols],
                kv[p].at[pl.ds(me * blocks_here + r * half, half), kind],
                side_sem.at[p, kind],
                link_sem.at[p, me],
                beside,
                r,
            )
            for kind, source in enumerate((ck_in, cv_in))
        ]

    def feeds():
        todo = []

        def add(cond, grp, other, ctx, slot):
            head = 2 * (1 - y if other else y) + grp
            place = 2 * grp + slot
            near = slot == 0
            items = [
                (
                    q_in.at[:, :, aligned(head, width)],
                    qs.at[place],
                    q_send.at[2 * grp + other],
                    q_recv.at[place],
                )
            ]
            for kind, source in enumerate((pk_in, pv_in)):
                items.append(
                    (
                        source.at[:, :, aligned(head, HEAD_WIDTH)],
                        own.at[place, kind, r],
                        own_send.at[4 * grp + 2 * other + kind],
                        own_recv.at[place, kind, r],
                    )
                )
            for src, dst, send, recv in items:
                if near:
                    todo.append((cond, pltpu.make_async_copy(src, dst, recv), True, (grp, other)))
                else:
                    copy = remote(src, dst, send, recv, ctx, r)
                    todo.append((cond, copy, False, (grp, other)))

        add(None, 0, 0, me, 0)
        add(None, 0, 1, beside, 1)
        add(is_inner, 1, 0, me, 0)
        add(is_inner, 1, 1, beside, 1)
        add(is_outer, 1, 0, z_twin * 2 + y, 2)
        add(is_outer, 1, 1, z_twin * 2 + 1 - y, 3)
        return todo

    def pass_own(place):
        return [
            remote(
                own.at[place, kind, 0],
                own.at[place, kind, 0],
                pass_send.at[place, kind],
                own_recv.at[place, kind, 0],
                me,
                1,
            )
            for kind in range(2)
        ]

    def table_copies():
        return [
            (None, remote(table_in, table.at[1], table_send.at[0], table_recv.at[1], beside, r)),
            (
                is_outer,
                remote(
                    table_in, table.at[2], table_send.at[1], table_recv.at[2], z_twin * 2 + y, r
                ),
            ),
            (
                is_outer,
                remote(
                    table_in, table.at[3], table_send.at[2], table_recv.at[3], z_twin * 2 + 1 - y, r
                ),
            ),
        ]

    def guarded(cond, action):
        if cond is None:
            action()
        else:
            pl.when(cond)(action)

    def ahead_copy(p, j):
        ctx = chunk_at(j)
        return remote(
            lane(p, ctx, r), lane(p, ctx, r), ahead_sem.at[p, j], link_sem.at[p, ctx],
            z_ahead * 2 + y, r,
        )

    def back_copy(p, j):
        ctx = chunk_at(j)
        return remote(
            lane(p, ctx, r), lane(p, ctx, r), back_sem.at[p, j], link_sem.at[p, ctx],
            z_twin * 2 + y, r,
        )

    def twin_copy(p, j):
        ctx = chunk_at(j)
        return remote(
            lane(p, ctx, r), lane(p, ctx, r), twin_sem.at[p, j], twin_recv.at[p, ctx], me, 1 - r
        )

    def goes(p, j):
        found = [(j < 2 + 2 * inner, ahead_copy(p, j))]
        if p < 2:
            found.append((is_inner & ((j < 2) | (j >= 4)), back_copy(p, j)))
        return found

    def relay(p, j, hold=False):
        ctx = chunk_at(j)
        ref = lane(p, ctx, r)
        remote(ref, ref, twin_sem.at[p, j], link_sem.at[p, ctx], me, 1 - r).wait_recv()
        for cond, copy in goes(p, j)[1 if hold else 0 :]:
            guarded(cond, copy.start)
        guarded(None if p < 2 else is_inner, twin_copy(p, j).start)

    def push(p, j):
        cond, copy = goes(p, j)[0]
        guarded(cond, copy.start)

    def load(p):
        loads[2 * p].wait()
        loads[2 * p + 1].wait()

    def complete(p):
        def one(j, carry):
            ctx = chunk_at(j)
            remote(
                lane(p, ctx, 1 - r), lane(p, ctx, 1 - r), twin_sem.at[p, j], twin_recv.at[p, ctx],
                me, 1 - r,
            ).wait_recv()
            return carry

        lax.fori_loop(1, CHUNKS, one, 0)

    todo = feeds()

    def feed(grp, other):
        for item in todo:
            if not item[2] and item[3] == (grp, other):
                guarded(item[0], item[1].start)

    for item in todo:
        if item[2]:
            guarded(item[0], item[1].start)
    for copy in side_copies(0):
        copy.start()
    for cond, copy in table_copies():
        guarded(cond, copy.start)
    load(0)
    push(0, 0)
    for copy in side_copies(1):
        copy.start()
    feed(0, 1)
    for p in range(1, PHASES):
        load(p)

    @pl.when(is_inner)
    def _():
        back_copy(0, 0).start()
        back_copy(1, 0).start()

    for copy in side_copies(2) + side_copies(3):
        copy.start()

    @pl.when(is_inner)
    def _():
        feed(1, 1)

    def await_slot(place):
        pltpu.make_async_copy(qs.at[place], qs.at[place], q_recv.at[place]).wait()
        for kind in range(2):
            ref = own.at[place, kind, r]
            pltpu.make_async_copy(ref, ref, own_recv.at[place, kind, r]).wait()

        @pl.when(r == 0)
        def _():
            for copy in pass_own(place):
                copy.start()

        @pl.when(r == 1)
        def _():
            for kind in range(2):
                ref = own.at[place, kind, 0]
                pltpu.make_async_copy(ref, ref, own_recv.at[place, kind, 0]).wait()

    def query(t, u):
        return qs[t // count, t % count, :, u * HEAD_WIDTH : (u + 1) * HEAD_WIDTH]

    def own_unit(t):
        place, b = t // count, t % count

        def attend(earlier):
            row = lax.broadcasted_iota(jnp.int32, (ROWS, ROWS), 0)
            column = lax.broadcasted_iota(jnp.int32, (ROWS, ROWS), 1)
            for u in range(group):
                parts = [jnp.where(column <= row, score(query(t, u), own[place, 0, r, b]), NEGATIVE)]
                values = [own[place, 1, r, b]]
                if earlier:
                    parts.append(score(query(t, u), own[place, 0, 0, b]))
                    values.append(own[place, 1, 0, b])
                stat[t, u], acc[t, u] = fold(parts, values, None, None)

        pl.when(r == 0)(lambda: attend(False))
        pl.when(r == 1)(lambda: attend(True))

    def pick_unit(p, t):
        place, b = t // count, t % count
        grp, last = p // 2, p % 2 == 1
        slot = place - 2 * grp
        head = (2 * y + grp) * group
        for u in range(group):
            at = (b * query_heads + head + u) * 2
            first = picked[slot, 0, at]
            second = picked[slot, 0, at + 1]
            rows = query(t, u)
            peak, mixed = fold(
                [score(rows, kv[p][first, 0]), score(rows, kv[p][second, 0])],
                [kv[p][first, 1], kv[p][second, 1]],
                stat[t, u],
                acc[t, u],
            )
            if last:
                share = mixed[:, :HEAD_WIDTH] / mixed[:, HEAD_WIDTH:]
                ans[t, :, u * HEAD_WIDTH : (u + 1) * HEAD_WIDTH] = share.astype(ans.dtype)
            else:
                stat[t, u] = peak
                acc[t, u] = mixed

    def answer(t, grp, act_near, act_far):
        place, b = t // count, t % count
        slot = place - 2 * grp
        head = 2 * y + grp
        target = out.at[b, :, aligned(head, width)]
        zt = z + (slot // 2) * (z_twin - z)
        ctx = zt * 2 + (y + slot % 2) % 2

        @pl.when(slot == 0)
        def _():
            act_near(pltpu.make_async_copy(ans.at[t], target, ans_send.at[t]))

        @pl.when(slot > 0)
        def _():
            act_far(
                remote(ans.at[t], target, ans_send.at[t], ans_recv.at[head * count + b], ctx, r)
            )

    def send_answer(grp, t):
        answer(t, grp, lambda c: c.start(), lambda c: c.start())

    def stage(first, units, unit, relays, after=None):
        def one(i, carry):
            unit(first + i)
            if after is not None:
                pl.when(i > 0)(lambda: after(first + i - 1))
            for k, act in enumerate(relays):
                pl.when(i == (k + 1) * units // len(relays) - 1)(act)
            return carry

        lax.fori_loop(0, units, one, 0)

    def chain(*steps):
        def act():
            for step in steps:
                step()

        return act

    def at(p, j, hold=False):
        return lambda: relay(p, j, hold)

    def own_slot(place, *relays):
        await_slot(place)
        stage(place * count, count, own_unit, relays)

    def picks(p, slot, slots, *relays):
        grp, last = p // 2, p % 2 == 1
        first, units = (2 * grp + slot) * count, slots * count
        after = functools.partial(send_answer, grp) if last else None
        stage(first, units, functools.partial(pick_unit, p), relays, after)
        if last:
            send_answer(grp, first + units - 1)

    pltpu.make_async_copy(table_in, table.at[0], table_recv.at[0]).start()

    def await_table(slots):
        for slot in range(slots):
            pltpu.make_async_copy(table.at[slot], table.at[slot], table_recv.at[slot]).wait()
        copy = pltpu.make_async_copy(
            table.at[pl.ds(0, slots)], picked.at[pl.ds(0, slots)], picked_sem.at[0]
        )
        copy.start()
        copy.wait()

    @pl.when(is_inner)
    def _():
        own_slot(0, at(0, 1))
        own_slot(2, at(0, 2), at(0, 3))
        push(1, 0)
        for p, j in ((1, 1), (0, 4), (0, 5), (1, 2), (0, 6), (1, 3), (0, 7)):
            relay(p, j)
        push(2, 0)
        await_table(4)
        own_slot(1)
        complete(0)
        picks(0, 0, 2, at(1, 4), at(2, 1), at(1, 5))
        own_slot(4, at(1, 6), at(3, 1, True))
        for p, j in ((2, 2), (1, 7)):
            relay(p, j)
        complete(1)
        push(3, 0)
        picks(1, 1, 1, at(2, 3))
        push(3, 1)
        picks(1, 0, 1, at(2, 4))
        own_slot(3, at(2, 5), at(2, 6))
        relay(2, 7)
        complete(2)
        picks(2, 0, 3, at(3, 2), at(3, 4), at(3, 3))
        own_slot(5, at(3, 5))
        picks(2, 3, 1, at(3, 6))
        relay(3, 7)
        complete(3)
        picks(3, 2, 2)
        picks(3, 1, 1)
        picks(3, 0, 1)

    @pl.when(is_outer)
    def _():
        own_slot(0, at(0, 1))
        push(1, 0)
        relay(1, 1)
        feed(1, 0)
        push(2, 0)
        await_table(2)
        own_slot(1)
        relay(2, 1)
        feed(1, 1)
        push(3, 0)
        relay(3, 1)
        lax.fori_loop(2, CHUNKS, lambda j, c: (relay(0, j), c)[1], 0)
        complete(0)
        picks(0, 0, 2, *[at(1, j) for j in range(2, 5)])
        lax.fori_loop(5, CHUNKS, lambda j, c: (relay(1, j), c)[1], 0)
        complete(1)
        picks(1, 1, 1)
        picks(1, 0, 1)

    for item in todo:
        if not item[2]:
            guarded(item[0], item[1].wait_send)
    for cond, copy in table_copies():
        guarded(cond, copy.wait_send)
    for p in range(PHASES):
        for copy in side_copies(p):
            copy.wait_send()

        def drain(j, carry):
            for cond, copy in goes(p, j):
                guarded(cond, copy.wait_send)
            twin = j >= 1 if p < 2 else (j >= 1) & is_inner
            guarded(twin, twin_copy(p, j).wait_send)
            return carry

        lax.fori_loop(0, CHUNKS, drain, 0)

    for place in range(6):
        sent = r == 0 if place < 2 else (r == 0) & is_inner

        @pl.when(sent)
        def _():
            for copy in pass_own(place):
                copy.wait_send()

    def settle(grp, t, carry):
        answer(t, grp, lambda c: c.wait(), lambda c: c.wait_send())
        return carry

    lax.fori_loop(0, 2 * count, functools.partial(settle, 0), 0)

    @pl.when(is_inner)
    def _():
        lax.fori_loop(2 * count, 6 * count, functools.partial(settle, 1), 0)

    def landed(k, carry):
        head, b = k // count, k % count
        target = out.at[b, :, aligned(head, width)]
        near = (head // 2 == y) & ((head % 2 == 0) | is_inner)

        @pl.when(jnp.logical_not(near))
        def _():
            remote(target, target, ans_send.at[0], ans_recv.at[k], me, 1 - r).wait_recv()

        return carry

    lax.fori_loop(0, 4 * count, landed, 0)


def spread_body(queries, prefill_keys, prefill_values, context_keys, context_values, picks):
    count, height, full = queries.shape
    key_heads = prefill_keys.shape[2] // HEAD_WIDTH
    group = full // prefill_keys.shape[2]
    blocks_here = context_keys.shape[0] // BLOCK_TOKENS
    blocks = blocks_here * CHUNKS
    units = 6 * count
    lanes = 2 * count * picks.shape[1]
    flat = picks[:, :, :2].reshape(1, lanes).astype(jnp.int32)
    table = jnp.pad(flat, ((0, 7), (0, -lanes % HEAD_WIDTH)))
    split = (blocks_here, 2, ROWS, context_keys.shape[1])
    dma = pltpu.SemaphoreType.DMA
    anywhere = pl.BlockSpec(memory_space=pl.ANY)
    work = (2 * LINE + 4 * 4) * count * group * key_heads // 4
    return pl.pallas_call(
        span_kernel,
        out_shape=jax.ShapeDtypeStruct(queries.shape, queries.dtype),
        in_specs=[anywhere] * 6,
        out_specs=anywhere,
        scratch_shapes=[pltpu.VMEM((blocks, 2, ROWS, HEAD_WIDTH), jnp.bfloat16)] * PHASES
        + [
            pltpu.VMEM((6, count, height, group * HEAD_WIDTH), jnp.bfloat16),
            pltpu.VMEM((6, 2, 2, count, height, HEAD_WIDTH), jnp.bfloat16),
            pltpu.VMEM((4,) + table.shape, jnp.int32),
            pltpu.SMEM((4,) + table.shape, jnp.int32),
            pltpu.VMEM((units, group, height, 2 * HEAD_WIDTH), jnp.float32),
            pltpu.VMEM((units, group, height, HEAD_WIDTH), jnp.float32),
            pltpu.VMEM((units, height, group * HEAD_WIDTH), jnp.bfloat16),
            dma((PHASES, CHUNKS)),
            dma((PHASES, CHUNKS)),
            dma((PHASES, CHUNKS)),
            dma((PHASES, CHUNKS)),
            dma((PHASES, CHUNKS)),
            dma((PHASES, 2)),
            dma((PHASES, 2)),
            dma((4,)),
            dma((6,)),
            dma((8,)),
            dma((6, 2)),
            dma((6, 2, 2)),
            dma((3,)),
            dma((4,)),
            dma((1,)),
            dma((units,)),
            dma((4 * count,)),
        ],
        compiler_params=pltpu.CompilerParams(
            collective_id=0, has_side_effects=True, vmem_limit_bytes=60 * 2**20
        ),
        cost_estimate=pl.CostEstimate(
            flops=work * 4 * ROWS * BLOCK_TOKENS * HEAD_WIDTH,
            transcendentals=work * ROWS * BLOCK_TOKENS,
            bytes_accessed=24 * 2**20,
        ),
        name="spread_attend",
    )(
        table,
        queries,
        prefill_keys,
        prefill_values,
        context_keys.reshape(split),
        context_values.reshape(split),
    )


def body(*args):
    queries, prefill_keys, _, context_keys, _, _ = args
    key_heads = prefill_keys.shape[2] // HEAD_WIDTH
    fits = lax.axis_size("ctx") == CHUNKS and lax.axis_size("rep") == 2 and key_heads == 4
    fits = fits and queries.shape[1] == ROWS and context_keys.shape[0] % (2 * BLOCK_TOKENS) == 0
    if fits:
        return spread_body(*args)
    return routed_body(*args)


def solution(mesh):
    return jax.shard_map(
        body,
        mesh=mesh,
        in_specs=(
            P(("groups", "ctx"), "rep", "head"),
            P(("groups", "ctx"), "rep", "head"),
            P(("groups", "ctx"), "rep", "head"),
            P(("groups", "ctx"), "head"),
            P(("groups", "ctx"), "head"),
            P(("groups", "ctx"), "head", None),
        ),
        out_specs=P(("groups", "ctx"), "rep", "head"),
        check_vma=False,
    )
```

```python
import functools
import math

import jax
import jax.numpy as jnp
from jax import lax
from jax.experimental import pallas as pl
from jax.experimental.pallas import tpu as pltpu
from jax.sharding import PartitionSpec as P


HEAD_WIDTH = 128
BLOCK_TOKENS = 512


NEGATIVE = -1e30


def from_behind(value, axis, steps):
    count = lax.axis_size(axis)
    first, last = (max(0, -steps), min(count, count - steps))
    return lax.ppermute(value, axis, [(source, source + steps) for source in range(first, last)])


def partial_attention(scores, values, allowed, pattern):
    scores = jnp.where(allowed, scores, NEGATIVE)
    highest = jnp.max(scores, axis=-1, keepdims=True)
    weights = jnp.exp(scores - highest)
    totals = jnp.sum(weights, axis=-1, keepdims=True)
    mixed = jnp.einsum(
        pattern, weights.astype(jnp.bfloat16), values, preferred_element_type=jnp.float32
    )
    return (mixed / totals, highest[..., 0] + jnp.log(totals[..., 0]))


def assign_slots(chosen, blocks_here, capacity):
    flat = chosen.reshape(-1)
    holders = flat // blocks_here
    places = jnp.arange(flat.shape[0])
    earlier = jnp.sum(
        (holders[:, None] == holders[None, :]) & (places[None, :] < places[:, None]), axis=1
    )
    return (holders * capacity + earlier, flat - holders * blocks_here)


def routed_body(queries, prefill_keys, prefill_values, context_keys, context_values, picks):
    local_count = queries.shape[0]
    stack_height = queries.shape[1]
    query_heads = queries.shape[2] // HEAD_WIDTH
    key_heads = prefill_keys.shape[2] // HEAD_WIDTH
    head_grouping = query_heads // key_heads
    blocks_here = context_keys.shape[0] // BLOCK_TOKENS
    ctx_size = lax.axis_size("ctx")
    pick_count = 2 * local_count * query_heads
    capacity = max(2, 2 * pick_count // ctx_size)
    slot_count = ctx_size * capacity
    scale = HEAD_WIDTH ** (-0.5)
    rep_index = lax.axis_index("rep")
    earlier_keys, earlier_values = from_behind((prefill_keys, prefill_values), "rep", 1)
    selected_block_keys = jnp.concatenate([earlier_keys, prefill_keys], 1).reshape(
        local_count, 2 * stack_height, key_heads, HEAD_WIDTH
    )
    selected_block_values = jnp.concatenate([earlier_values, prefill_values], 1).reshape(
        local_count, 2 * stack_height, key_heads, HEAD_WIDTH
    )
    grouped = queries.reshape(local_count, stack_height, key_heads, head_grouping, HEAD_WIDTH)
    query_place = rep_index * stack_height + jnp.arange(stack_height)
    key_place = (rep_index - 1) * stack_height + jnp.arange(2 * stack_height)
    allowed = (key_place[None, :] <= query_place[:, None]) & (key_place[None, :] >= 0)

    def own_block(paired):
        rows_here, keys_here, values_here = paired
        scores = (
            jnp.einsum("rkgd,jkd->kgrj", rows_here, keys_here, preferred_element_type=jnp.float32)
            * scale
        )
        return partial_attention(scores, values_here, allowed, "kgrj,jkd->kgrd")

    own_mixed, own_log = lax.map(own_block, (grouped, selected_block_keys, selected_block_values))
    own_mixed = own_mixed.reshape(local_count, query_heads, stack_height, HEAD_WIDTH)
    own_log = own_log.reshape(local_count, query_heads, stack_height)
    targets, local_blocks = assign_slots(picks[:, :, :2], blocks_here, capacity)
    routing = targets[:, None] == jnp.arange(slot_count)[None, :]
    sending = routing.astype(jnp.bfloat16).reshape(local_count, query_heads, 2, slot_count)
    by_head = queries.reshape(local_count, stack_height, query_heads, HEAD_WIDTH)
    outbound = jnp.einsum("qhps,qrhd->srd", sending, by_head, preferred_element_type=jnp.float32)
    outbound = outbound.astype(jnp.bfloat16).reshape(ctx_size, capacity, stack_height, HEAD_WIDTH)
    pick_heads = jnp.arange(pick_count) // 2 % query_heads // head_grouping
    key_tiles = context_keys.reshape(blocks_here, BLOCK_TOKENS, key_heads, HEAD_WIDTH)
    value_tiles = context_values.reshape(blocks_here, BLOCK_TOKENS, key_heads, HEAD_WIDTH)
    block_label = jnp.sum(jnp.where(routing, local_blocks[:, None], 0), axis=0)
    head_label = jnp.sum(jnp.where(routing, pick_heads[:, None], 0), axis=0)
    labels = jnp.stack([block_label, head_label], axis=-1).reshape(ctx_size, capacity, 2)
    inbound = lax.all_to_all(outbound, "ctx", split_axis=0, concat_axis=0, tiled=True)
    arrived = lax.all_to_all(labels, "ctx", split_axis=0, concat_axis=0, tiled=True)
    leading = inbound.shape[:2]

    def single(paired):
        rows_in, position = paired
        anchor = (position[0], 0, position[1], 0)
        keys_tile = lax.dynamic_slice(key_tiles, anchor, (1, BLOCK_TOKENS, 1, HEAD_WIDTH)).reshape(
            BLOCK_TOKENS, HEAD_WIDTH
        )
        values_tile = lax.dynamic_slice(
            value_tiles, anchor, (1, BLOCK_TOKENS, 1, HEAD_WIDTH)
        ).reshape(BLOCK_TOKENS, HEAD_WIDTH)
        scores = (
            lax.dot_general(
                rows_in, keys_tile, (((1,), (1,)), ((), ())), preferred_element_type=jnp.float32
            )
            * scale
        )
        mixed, logged = partial_attention(scores, values_tile, True, "rj,jd->rd")
        return (mixed.astype(jnp.bfloat16), logged)

    flat_rows = inbound.reshape((-1,) + inbound.shape[2:])
    flat_labels = arrived.reshape(-1, 2)
    mixed, logged = lax.map(single, (flat_rows, flat_labels), batch_size=8)
    served = mixed.reshape(leading + mixed.shape[1:])
    served_logs = logged.reshape(leading + logged.shape[1:])
    answers = lax.all_to_all(served, "ctx", split_axis=0, concat_axis=0, tiled=True)
    answer_logs = lax.all_to_all(served_logs, "ctx", split_axis=0, concat_axis=0, tiled=True)
    gathered = answers.reshape(slot_count, stack_height, HEAD_WIDTH)[targets]
    gathered_logs = answer_logs.reshape(slot_count, stack_height)[targets]
    remote_mixed = gathered.astype(jnp.float32).reshape(
        local_count, query_heads, 2, stack_height, HEAD_WIDTH
    )
    remote_logs = gathered_logs.reshape(local_count, query_heads, 2, stack_height)
    all_logs = jnp.concatenate([own_log[:, :, None], remote_logs], axis=2)
    all_mixed = jnp.concatenate([own_mixed[:, :, None], remote_mixed], axis=2)
    peak = jnp.max(all_logs, axis=2, keepdims=True)
    shares = jnp.exp(all_logs - peak)
    merged = jnp.sum(shares[..., None] * all_mixed, axis=2) / jnp.sum(shares, axis=2)[..., None]
    return (
        jnp.transpose(merged, (0, 2, 1, 3))
        .reshape(local_count, stack_height, query_heads * HEAD_WIDTH)
        .astype(jnp.bfloat16)
    )


RATE = HEAD_WIDTH ** (-0.5) * math.log2(math.e)
MESH = pl.DeviceIdType.MESH
LINE = 4
ROWS = BLOCK_TOKENS // 2
PHASES = 4
CHUNKS = 2 * LINE


def score(rows, keys):
    return lax.dot_general(
        rows, keys, (((1,), (1,)), ((), ())), preferred_element_type=jnp.float32
    )


def fold(parts, values, peak, mixed):
    highest = None
    for part in parts:
        for at in range(0, part.shape[1], HEAD_WIDTH):
            piece = part[:, at : at + HEAD_WIDTH]
            highest = piece if highest is None else jnp.maximum(highest, piece)
    highest = jnp.max(highest, axis=-1, keepdims=True)
    highest = jnp.broadcast_to(highest, (parts[0].shape[0], HEAD_WIDTH))
    if peak is not None:
        highest = jnp.maximum(peak, highest)
        fade = jnp.exp2((peak - highest) * RATE)
        mixed = mixed * jnp.concatenate([fade, fade], axis=1)
    level = highest * RATE
    for part, value in zip(parts, values):
        base = jnp.concatenate([level] * (part.shape[1] // HEAD_WIDTH), axis=1)
        weights = jnp.exp2(part * RATE - base).astype(jnp.bfloat16)
        beside = jnp.concatenate([value, jnp.ones_like(value)], axis=1)
        product = jnp.dot(weights, beside, preferred_element_type=jnp.float32)
        mixed = product if mixed is None else mixed + product
    return highest, mixed


def aligned(index, width):
    return pl.ds(pl.multiple_of(index * width, width), width)


def span_kernel(
    table_in,
    q_in,
    pk_in,
    pv_in,
    ck_in,
    cv_in,
    out,
    kv0,
    kv1,
    kv2,
    kv3,
    qs,
    own,
    table,
    picked,
    acc,
    stat,
    ans,
    ahead_sem,
    back_sem,
    twin_sem,
    link_sem,
    twin_recv,
    side_sem,
    load_sem,
    q_send,
    q_recv,
    own_send,
    pass_send,
    own_recv,
    table_send,
    table_recv,
    picked_sem,
    ans_send,
    ans_recv,
):
    kv = (kv0, kv1, kv2, kv3)
    me, r = lax.axis_index("ctx"), lax.axis_index("rep")
    z, y = me // 2, me % 2
    side = z // 2
    inner = (z + side) % 2
    z_twin = z + 1 - 2 * (z % 2)
    z_ahead = inner * (3 - z) + (1 - inner) * z_twin
    is_inner, is_outer = inner == 1, inner == 0
    group = q_in.shape[2] // pk_in.shape[2]
    width = group * HEAD_WIDTH
    blocks_here = ck_in.shape[0]
    half = blocks_here // 2
    count = q_in.shape[0]

    def remote(src, dst, send, recv, ctx, rep):
        return pltpu.make_async_remote_copy(
            src_ref=src,
            dst_ref=dst,
            send_sem=send,
            recv_sem=recv,
            device_id={"ctx": ctx, "rep": rep},
            device_id_type=MESH,
        )

    def chunk_at(j):
        jj = j // 2
        m = jj + inner * (1 - 2 * jj) * (1 - jj // 2)
        return (m + side * (3 - 2 * m)) * 2 + (y + j % 2) % 2

    def lane(p, ctx, rep):
        return kv[p].at[pl.ds(ctx * blocks_here + rep * half, half)]

    barrier = pltpu.get_barrier_semaphore()

    def greet(ctx, rep):
        pl.semaphore_signal(barrier, inc=1, device_id={"ctx": ctx, "rep": rep}, device_id_type=MESH)

    beside = z * 2 + 1 - y
    greet(me, 1 - r)
    greet(beside, r)
    greet(z_twin * 2 + y, r)
    greet(z_twin * 2 + 1 - y, r)

    loads = []
    for p in range(PHASES):
        cols = aligned(2 * y + p // 2, HEAD_WIDTH)
        for kind, source in enumerate((ck_in, cv_in)):
            loads.append(
                pltpu.make_async_copy(
                    source.at[:, p % 2, :, cols],
                    kv[p].at[pl.ds(me * blocks_here, blocks_here), kind],
                    load_sem.at[p, kind],
                )
            )
    for load in loads:
        load.start()

    @pl.when(is_inner)
    def _():
        greet((3 - z) * 2 + y, r)
        pl.semaphore_wait(barrier, 5)

    @pl.when(is_outer)
    def _():
        pl.semaphore_wait(barrier, 4)

    def side_copies(p):
        cols = aligned(2 * (1 - y) + p // 2, HEAD_WIDTH)
        return [
            remote(
                source.at[pl.ds(r * half, half), p % 2, :, cols],
                kv[p].at[pl.ds(me * blocks_here + r * half, half), kind],
                side_sem.at[p, kind],
                link_sem.at[p, me],
                beside,
                r,
            )
            for kind, source in enumerate((ck_in, cv_in))
        ]

    def feeds():
        todo = []

        def add(cond, grp, other, ctx, slot):
            head = 2 * (1 - y if other else y) + grp
            place = 2 * grp + slot
            near = slot == 0
            items = [
                (
                    q_in.at[:, :, aligned(head, width)],
                    qs.at[place],
                    q_send.at[2 * grp + other],
                    q_recv.at[place],
                )
            ]
            for kind, source in enumerate((pk_in, pv_in)):
                items.append(
                    (
                        source.at[:, :, aligned(head, HEAD_WIDTH)],
                        own.at[place, kind, r],
                        own_send.at[4 * grp + 2 * other + kind],
                        own_recv.at[place, kind, r],
                    )
                )
            for src, dst, send, recv in items:
                if near:
                    todo.append((cond, pltpu.make_async_copy(src, dst, recv), True, (grp, other)))
                else:
                    copy = remote(src, dst, send, recv, ctx, r)
                    todo.append((cond, copy, False, (grp, other)))

        add(None, 0, 0, me, 0)
        add(None, 0, 1, beside, 1)
        add(is_inner, 1, 0, me, 0)
        add(is_inner, 1, 1, beside, 1)
        add(is_outer, 1, 0, z_twin * 2 + y, 2)
        add(is_outer, 1, 1, z_twin * 2 + 1 - y, 3)
        return todo

    def pass_own(place):
        return [
            remote(
                own.at[place, kind, 0],
                own.at[place, kind, 0],
                pass_send.at[place, kind],
                own_recv.at[place, kind, 0],
                me,
                1,
            )
            for kind in range(2)
        ]

    def table_copies():
        return [
            (None, remote(table_in, table.at[1], table_send.at[0], table_recv.at[1], beside, r)),
            (
                is_outer,
                remote(
                    table_in, table.at[2], table_send.at[1], table_recv.at[2], z_twin * 2 + y, r
                ),
            ),
            (
                is_outer,
                remote(
                    table_in, table.at[3], table_send.at[2], table_recv.at[3], z_twin * 2 + 1 - y, r
                ),
            ),
        ]

    def guarded(cond, action):
        if cond is None:
            action()
        else:
            pl.when(cond)(action)

    def ahead_copy(p, j):
        ctx = chunk_at(j)
        return remote(
            lane(p, ctx, r), lane(p, ctx, r), ahead_sem.at[p, j], link_sem.at[p, ctx],
            z_ahead * 2 + y, r,
        )

    def back_copy(p, j):
        ctx = chunk_at(j)
        return remote(
            lane(p, ctx, r), lane(p, ctx, r), back_sem.at[p, j], link_sem.at[p, ctx],
            z_twin * 2 + y, r,
        )

    def twin_copy(p, j):
        ctx = chunk_at(j)
        return remote(
            lane(p, ctx, r), lane(p, ctx, r), twin_sem.at[p, j], twin_recv.at[p, ctx], me, 1 - r
        )

    def goes(p, j):
        found = [(j < 2 + 2 * inner, ahead_copy(p, j))]
        if p < 2:
            found.append((is_inner & ((j < 2) | (j >= 4)), back_copy(p, j)))
        return found

    def relay(p, j, hold=False):
        ctx = chunk_at(j)
        ref = lane(p, ctx, r)
        remote(ref, ref, twin_sem.at[p, j], link_sem.at[p, ctx], me, 1 - r).wait_recv()
        for cond, copy in goes(p, j)[1 if hold else 0 :]:
            guarded(cond, copy.start)
        guarded(None if p < 2 else is_inner, twin_copy(p, j).start)

    def push(p, j):
        cond, copy = goes(p, j)[0]
        guarded(cond, copy.start)

    def load(p):
        loads[2 * p].wait()
        loads[2 * p + 1].wait()

    def complete(p):
        def one(j, carry):
            ctx = chunk_at(j)
            remote(
                lane(p, ctx, 1 - r), lane(p, ctx, 1 - r), twin_sem.at[p, j], twin_recv.at[p, ctx],
                me, 1 - r,
            ).wait_recv()
            return carry

        lax.fori_loop(1, CHUNKS, one, 0)

    todo = feeds()

    def feed(grp, other):
        for item in todo:
            if not item[2] and item[3] == (grp, other):
                guarded(item[0], item[1].start)

    for item in todo:
        if item[2]:
            guarded(item[0], item[1].start)
    for copy in side_copies(0):
        copy.start()
    for cond, copy in table_copies():
        guarded(cond, copy.start)
    load(0)
    push(0, 0)
    for copy in side_copies(1):
        copy.start()
    load(1)
    push(1, 0)
    feed(0, 1)
    load(2)
    load(3)

    @pl.when(is_inner)
    def _():
        back_copy(0, 0).start()
        back_copy(1, 0).start()

    for copy in side_copies(2) + side_copies(3):
        copy.start()

    @pl.when(is_inner)
    def _():
        feed(1, 1)

    def await_slot(place):
        pltpu.make_async_copy(qs.at[place], qs.at[place], q_recv.at[place]).wait()
        for kind in range(2):
            ref = own.at[place, kind, r]
            pltpu.make_async_copy(ref, ref, own_recv.at[place, kind, r]).wait()

        @pl.when(r == 0)
        def _():
            for copy in pass_own(place):
                copy.start()

        @pl.when(r == 1)
        def _():
            for kind in range(2):
                ref = own.at[place, kind, 0]
                pltpu.make_async_copy(ref, ref, own_recv.at[place, kind, 0]).wait()

    def query(t, u):
        return qs[t // count, t % count, :, u * HEAD_WIDTH : (u + 1) * HEAD_WIDTH]

    def own_unit(t):
        place, b = t // count, t % count

        def attend(earlier):
            row = lax.broadcasted_iota(jnp.int32, (ROWS, ROWS), 0)
            column = lax.broadcasted_iota(jnp.int32, (ROWS, ROWS), 1)
            for u in range(group):
                parts = [jnp.where(column <= row, score(query(t, u), own[place, 0, r, b]), NEGATIVE)]
                values = [own[place, 1, r, b]]
                if earlier:
                    parts.append(score(query(t, u), own[place, 0, 0, b]))
                    values.append(own[place, 1, 0, b])
                stat[t, u], acc[t, u] = fold(parts, values, None, None)

        pl.when(r == 0)(lambda: attend(False))
        pl.when(r == 1)(lambda: attend(True))

    def pick_unit(p, t):
        place, b = t // count, t % count
        grp, last = p // 2, p % 2 == 1
        slot = place - 2 * grp
        head = (2 * y + grp) * group
        for u in range(group):
            first = picked[slot, 0, b, head + u]
            second = picked[slot, 1, b, head + u]
            rows = query(t, u)
            peak, mixed = fold(
                [score(rows, kv[p][first, 0]), score(rows, kv[p][second, 0])],
                [kv[p][first, 1], kv[p][second, 1]],
                stat[t, u],
                acc[t, u],
            )
            if last:
                share = mixed[:, :HEAD_WIDTH] / mixed[:, HEAD_WIDTH:]
                ans[t, :, u * HEAD_WIDTH : (u + 1) * HEAD_WIDTH] = share.astype(ans.dtype)
            else:
                stat[t, u] = peak
                acc[t, u] = mixed

    def answer(t, grp, act_near, act_far):
        place, b = t // count, t % count
        slot = place - 2 * grp
        head = 2 * y + grp
        target = out.at[b, :, aligned(head, width)]
        zt = z + (slot // 2) * (z_twin - z)
        ctx = zt * 2 + (y + slot % 2) % 2

        @pl.when(slot == 0)
        def _():
            act_near(pltpu.make_async_copy(ans.at[t], target, ans_send.at[t]))

        @pl.when(slot > 0)
        def _():
            act_far(
                remote(ans.at[t], target, ans_send.at[t], ans_recv.at[head * count + b], ctx, r)
            )

    def send_answer(grp, t):
        answer(t, grp, lambda c: c.start(), lambda c: c.start())

    def stage(first, units, unit, relays, after=None):
        def one(i, carry):
            unit(first + i)
            if after is not None:
                pl.when(i > 0)(lambda: after(first + i - 1))
            for k, act in enumerate(relays):
                pl.when(i == (k + 1) * units // len(relays) - 1)(act)
            return carry

        lax.fori_loop(0, units, one, 0)

    def chain(*steps):
        def act():
            for step in steps:
                step()

        return act

    def at(p, j, hold=False):
        return lambda: relay(p, j, hold)

    def own_slot(place, *relays):
        await_slot(place)
        stage(place * count, count, own_unit, relays)

    def picks(p, slot, slots, *relays):
        grp, last = p // 2, p % 2 == 1
        first, units = (2 * grp + slot) * count, slots * count
        after = functools.partial(send_answer, grp) if last else None
        stage(first, units, functools.partial(pick_unit, p), relays, after)
        if last:
            send_answer(grp, first + units - 1)

    pltpu.make_async_copy(table_in, table.at[0], table_recv.at[0]).start()

    def await_table(slots):
        for slot in range(slots):
            pltpu.make_async_copy(table.at[slot], table.at[slot], table_recv.at[slot]).wait()
        copy = pltpu.make_async_copy(
            table.at[pl.ds(0, slots)], picked.at[pl.ds(0, slots)], picked_sem.at[0]
        )
        copy.start()
        copy.wait()

    @pl.when(is_inner)
    def _():
        own_slot(0, at(0, 1))
        own_slot(2, at(0, 2), at(0, 3))
        for p, j in ((0, 4), (1, 1), (1, 2), (1, 4), (0, 5), (1, 3), (0, 6)):
            relay(p, j)
        push(2, 0)
        relay(0, 7)
        await_table(4)
        own_slot(1)
        complete(0)
        picks(0, 0, 2, at(1, 5), at(2, 1), at(2, 2), at(1, 6))
        push(3, 0)
        relay(1, 7)
        complete(1)
        picks(1, 1, 1, at(3, 1, True))
        picks(1, 0, 1, at(2, 4))
        own_slot(4, at(2, 3), chain(lambda: push(3, 1), at(3, 2)))
        own_slot(3, at(2, 5), at(3, 3))
        relay(2, 6)
        relay(2, 7)
        complete(2)
        picks(2, 0, 3, at(3, 4))
        own_slot(5, at(3, 5))
        picks(2, 3, 1, at(3, 6))
        relay(3, 7)
        complete(3)
        picks(3, 2, 2)
        picks(3, 1, 1)
        picks(3, 0, 1)

    @pl.when(is_outer)
    def _():
        own_slot(0, at(0, 1))
        relay(1, 1)
        push(2, 0)
        push(3, 0)
        feed(1, 0)
        await_table(2)
        own_slot(1)
        relay(2, 1)
        relay(3, 1)
        feed(1, 1)
        lax.fori_loop(2, CHUNKS, lambda j, c: (relay(0, j), c)[1], 0)
        complete(0)
        picks(0, 0, 2, *[at(1, j) for j in range(2, 5)])
        lax.fori_loop(5, CHUNKS, lambda j, c: (relay(1, j), c)[1], 0)
        complete(1)
        picks(1, 1, 1)
        picks(1, 0, 1)

    for item in todo:
        if not item[2]:
            guarded(item[0], item[1].wait_send)
    for cond, copy in table_copies():
        guarded(cond, copy.wait_send)
    for p in range(PHASES):
        for copy in side_copies(p):
            copy.wait_send()

        def drain(j, carry):
            for cond, copy in goes(p, j):
                guarded(cond, copy.wait_send)
            twin = j >= 1 if p < 2 else (j >= 1) & is_inner
            guarded(twin, twin_copy(p, j).wait_send)
            return carry

        lax.fori_loop(0, CHUNKS, drain, 0)

    for place in range(6):
        sent = r == 0 if place < 2 else (r == 0) & is_inner

        @pl.when(sent)
        def _():
            for copy in pass_own(place):
                copy.wait_send()

    def settle(grp, t, carry):
        answer(t, grp, lambda c: c.wait(), lambda c: c.wait_send())
        return carry

    lax.fori_loop(0, 2 * count, functools.partial(settle, 0), 0)

    @pl.when(is_inner)
    def _():
        lax.fori_loop(2 * count, 6 * count, functools.partial(settle, 1), 0)

    def landed(k, carry):
        head, b = k // count, k % count
        target = out.at[b, :, aligned(head, width)]
        near = (head // 2 == y) & ((head % 2 == 0) | is_inner)

        @pl.when(jnp.logical_not(near))
        def _():
            remote(target, target, ans_send.at[0], ans_recv.at[k], me, 1 - r).wait_recv()

        return carry

    lax.fori_loop(0, 4 * count, landed, 0)


def spread_body(queries, prefill_keys, prefill_values, context_keys, context_values, picks):
    count, height, full = queries.shape
    key_heads = prefill_keys.shape[2] // HEAD_WIDTH
    group = full // prefill_keys.shape[2]
    blocks_here = context_keys.shape[0] // BLOCK_TOKENS
    blocks = blocks_here * CHUNKS
    units = 6 * count
    table = jnp.transpose(picks, (2, 0, 1))
    split = (blocks_here, 2, ROWS, context_keys.shape[1])
    dma = pltpu.SemaphoreType.DMA
    anywhere = pl.BlockSpec(memory_space=pl.ANY)
    work = (2 * LINE + 4 * 4) * count * group * key_heads // 4
    return pl.pallas_call(
        span_kernel,
        out_shape=jax.ShapeDtypeStruct(queries.shape, queries.dtype),
        in_specs=[anywhere] * 6,
        out_specs=anywhere,
        scratch_shapes=[pltpu.VMEM((blocks, 2, ROWS, HEAD_WIDTH), jnp.bfloat16)] * PHASES
        + [
            pltpu.VMEM((6, count, height, group * HEAD_WIDTH), jnp.bfloat16),
            pltpu.VMEM((6, 2, 2, count, height, HEAD_WIDTH), jnp.bfloat16),
            pltpu.VMEM((4,) + table.shape, jnp.int32),
            pltpu.SMEM((4,) + table.shape, jnp.int32),
            pltpu.VMEM((units, group, height, 2 * HEAD_WIDTH), jnp.float32),
            pltpu.VMEM((units, group, height, HEAD_WIDTH), jnp.float32),
            pltpu.VMEM((units, height, group * HEAD_WIDTH), jnp.bfloat16),
            dma((PHASES, CHUNKS)),
            dma((PHASES, CHUNKS)),
            dma((PHASES, CHUNKS)),
            dma((PHASES, CHUNKS)),
            dma((PHASES, CHUNKS)),
            dma((PHASES, 2)),
            dma((PHASES, 2)),
            dma((4,)),
            dma((6,)),
            dma((8,)),
            dma((6, 2)),
            dma((6, 2, 2)),
            dma((3,)),
            dma((4,)),
            dma((1,)),
            dma((units,)),
            dma((4 * count,)),
        ],
        compiler_params=pltpu.CompilerParams(
            collective_id=0, has_side_effects=True, vmem_limit_bytes=60 * 2**20
        ),
        cost_estimate=pl.CostEstimate(
            flops=work * 4 * ROWS * BLOCK_TOKENS * HEAD_WIDTH,
            transcendentals=work * ROWS * BLOCK_TOKENS,
            bytes_accessed=24 * 2**20,
        ),
        name="spread_attend",
    )(
        table,
        queries,
        prefill_keys,
        prefill_values,
        context_keys.reshape(split),
        context_values.reshape(split),
    )


def body(*args):
    queries, prefill_keys, _, context_keys, _, _ = args
    key_heads = prefill_keys.shape[2] // HEAD_WIDTH
    fits = lax.axis_size("ctx") == CHUNKS and lax.axis_size("rep") == 2 and key_heads == 4
    fits = fits and queries.shape[1] == ROWS and context_keys.shape[0] % (2 * BLOCK_TOKENS) == 0
    if fits:
        return spread_body(*args)
    return routed_body(*args)


def solution(mesh):
    return jax.shard_map(
        body,
        mesh=mesh,
        in_specs=(
            P(("groups", "ctx"), "rep", "head"),
            P(("groups", "ctx"), "rep", "head"),
            P(("groups", "ctx"), "rep", "head"),
            P(("groups", "ctx"), "head"),
            P(("groups", "ctx"), "head"),
            P(("groups", "ctx"), "head", None),
        ),
        out_specs=P(("groups", "ctx"), "rep", "head"),
        check_vma=False,
    )
```

```python
import functools
import math

import jax
import jax.numpy as jnp
from jax import lax
from jax.experimental import pallas as pl
from jax.experimental.pallas import tpu as pltpu
from jax.sharding import PartitionSpec as P


HEAD_WIDTH = 128
BLOCK_TOKENS = 512


NEGATIVE = -1e30


def from_behind(value, axis, steps):
    count = lax.axis_size(axis)
    first, last = (max(0, -steps), min(count, count - steps))
    return lax.ppermute(value, axis, [(source, source + steps) for source in range(first, last)])


def partial_attention(scores, values, allowed, pattern):
    scores = jnp.where(allowed, scores, NEGATIVE)
    highest = jnp.max(scores, axis=-1, keepdims=True)
    weights = jnp.exp(scores - highest)
    totals = jnp.sum(weights, axis=-1, keepdims=True)
    mixed = jnp.einsum(
        pattern, weights.astype(jnp.bfloat16), values, preferred_element_type=jnp.float32
    )
    return (mixed / totals, highest[..., 0] + jnp.log(totals[..., 0]))


def assign_slots(chosen, blocks_here, capacity):
    flat = chosen.reshape(-1)
    holders = flat // blocks_here
    places = jnp.arange(flat.shape[0])
    earlier = jnp.sum(
        (holders[:, None] == holders[None, :]) & (places[None, :] < places[:, None]), axis=1
    )
    return (holders * capacity + earlier, flat - holders * blocks_here)


def routed_body(queries, prefill_keys, prefill_values, context_keys, context_values, picks):
    local_count = queries.shape[0]
    stack_height = queries.shape[1]
    query_heads = queries.shape[2] // HEAD_WIDTH
    key_heads = prefill_keys.shape[2] // HEAD_WIDTH
    head_grouping = query_heads // key_heads
    blocks_here = context_keys.shape[0] // BLOCK_TOKENS
    ctx_size = lax.axis_size("ctx")
    pick_count = 2 * local_count * query_heads
    capacity = max(2, 2 * pick_count // ctx_size)
    slot_count = ctx_size * capacity
    scale = HEAD_WIDTH ** (-0.5)
    rep_index = lax.axis_index("rep")
    earlier_keys, earlier_values = from_behind((prefill_keys, prefill_values), "rep", 1)
    selected_block_keys = jnp.concatenate([earlier_keys, prefill_keys], 1).reshape(
        local_count, 2 * stack_height, key_heads, HEAD_WIDTH
    )
    selected_block_values = jnp.concatenate([earlier_values, prefill_values], 1).reshape(
        local_count, 2 * stack_height, key_heads, HEAD_WIDTH
    )
    grouped = queries.reshape(local_count, stack_height, key_heads, head_grouping, HEAD_WIDTH)
    query_place = rep_index * stack_height + jnp.arange(stack_height)
    key_place = (rep_index - 1) * stack_height + jnp.arange(2 * stack_height)
    allowed = (key_place[None, :] <= query_place[:, None]) & (key_place[None, :] >= 0)

    def own_block(paired):
        rows_here, keys_here, values_here = paired
        scores = (
            jnp.einsum("rkgd,jkd->kgrj", rows_here, keys_here, preferred_element_type=jnp.float32)
            * scale
        )
        return partial_attention(scores, values_here, allowed, "kgrj,jkd->kgrd")

    own_mixed, own_log = lax.map(own_block, (grouped, selected_block_keys, selected_block_values))
    own_mixed = own_mixed.reshape(local_count, query_heads, stack_height, HEAD_WIDTH)
    own_log = own_log.reshape(local_count, query_heads, stack_height)
    targets, local_blocks = assign_slots(picks[:, :, :2], blocks_here, capacity)
    routing = targets[:, None] == jnp.arange(slot_count)[None, :]
    sending = routing.astype(jnp.bfloat16).reshape(local_count, query_heads, 2, slot_count)
    by_head = queries.reshape(local_count, stack_height, query_heads, HEAD_WIDTH)
    outbound = jnp.einsum("qhps,qrhd->srd", sending, by_head, preferred_element_type=jnp.float32)
    outbound = outbound.astype(jnp.bfloat16).reshape(ctx_size, capacity, stack_height, HEAD_WIDTH)
    pick_heads = jnp.arange(pick_count) // 2 % query_heads // head_grouping
    key_tiles = context_keys.reshape(blocks_here, BLOCK_TOKENS, key_heads, HEAD_WIDTH)
    value_tiles = context_values.reshape(blocks_here, BLOCK_TOKENS, key_heads, HEAD_WIDTH)
    block_label = jnp.sum(jnp.where(routing, local_blocks[:, None], 0), axis=0)
    head_label = jnp.sum(jnp.where(routing, pick_heads[:, None], 0), axis=0)
    labels = jnp.stack([block_label, head_label], axis=-1).reshape(ctx_size, capacity, 2)
    inbound = lax.all_to_all(outbound, "ctx", split_axis=0, concat_axis=0, tiled=True)
    arrived = lax.all_to_all(labels, "ctx", split_axis=0, concat_axis=0, tiled=True)
    leading = inbound.shape[:2]

    def single(paired):
        rows_in, position = paired
        anchor = (position[0], 0, position[1], 0)
        keys_tile = lax.dynamic_slice(key_tiles, anchor, (1, BLOCK_TOKENS, 1, HEAD_WIDTH)).reshape(
            BLOCK_TOKENS, HEAD_WIDTH
        )
        values_tile = lax.dynamic_slice(
            value_tiles, anchor, (1, BLOCK_TOKENS, 1, HEAD_WIDTH)
        ).reshape(BLOCK_TOKENS, HEAD_WIDTH)
        scores = (
            lax.dot_general(
                rows_in, keys_tile, (((1,), (1,)), ((), ())), preferred_element_type=jnp.float32
            )
            * scale
        )
        mixed, logged = partial_attention(scores, values_tile, True, "rj,jd->rd")
        return (mixed.astype(jnp.bfloat16), logged)

    flat_rows = inbound.reshape((-1,) + inbound.shape[2:])
    flat_labels = arrived.reshape(-1, 2)
    mixed, logged = lax.map(single, (flat_rows, flat_labels), batch_size=8)
    served = mixed.reshape(leading + mixed.shape[1:])
    served_logs = logged.reshape(leading + logged.shape[1:])
    answers = lax.all_to_all(served, "ctx", split_axis=0, concat_axis=0, tiled=True)
    answer_logs = lax.all_to_all(served_logs, "ctx", split_axis=0, concat_axis=0, tiled=True)
    gathered = answers.reshape(slot_count, stack_height, HEAD_WIDTH)[targets]
    gathered_logs = answer_logs.reshape(slot_count, stack_height)[targets]
    remote_mixed = gathered.astype(jnp.float32).reshape(
        local_count, query_heads, 2, stack_height, HEAD_WIDTH
    )
    remote_logs = gathered_logs.reshape(local_count, query_heads, 2, stack_height)
    all_logs = jnp.concatenate([own_log[:, :, None], remote_logs], axis=2)
    all_mixed = jnp.concatenate([own_mixed[:, :, None], remote_mixed], axis=2)
    peak = jnp.max(all_logs, axis=2, keepdims=True)
    shares = jnp.exp(all_logs - peak)
    merged = jnp.sum(shares[..., None] * all_mixed, axis=2) / jnp.sum(shares, axis=2)[..., None]
    return (
        jnp.transpose(merged, (0, 2, 1, 3))
        .reshape(local_count, stack_height, query_heads * HEAD_WIDTH)
        .astype(jnp.bfloat16)
    )


RATE = HEAD_WIDTH ** (-0.5) * math.log2(math.e)
MESH = pl.DeviceIdType.MESH
LINE = 4
ROWS = BLOCK_TOKENS // 2
PHASES = 4
CHUNKS = 2 * LINE


def score(rows, keys):
    return lax.dot_general(
        rows, keys, (((1,), (1,)), ((), ())), preferred_element_type=jnp.float32
    )


def fold(parts, values, peak, mixed):
    highest = None
    for part in parts:
        for at in range(0, part.shape[1], HEAD_WIDTH):
            piece = part[:, at : at + HEAD_WIDTH]
            highest = piece if highest is None else jnp.maximum(highest, piece)
    highest = jnp.max(highest, axis=-1, keepdims=True)
    highest = jnp.broadcast_to(highest, (parts[0].shape[0], HEAD_WIDTH))
    if peak is not None:
        highest = jnp.maximum(peak, highest)
        fade = jnp.exp2((peak - highest) * RATE)
        mixed = mixed * jnp.concatenate([fade, fade], axis=1)
    level = highest * RATE
    for part, value in zip(parts, values):
        base = jnp.concatenate([level] * (part.shape[1] // HEAD_WIDTH), axis=1)
        weights = jnp.exp2(part * RATE - base).astype(jnp.bfloat16)
        beside = jnp.concatenate([value, jnp.ones_like(value)], axis=1)
        product = jnp.dot(weights, beside, preferred_element_type=jnp.float32)
        mixed = product if mixed is None else mixed + product
    return highest, mixed


def aligned(index, width):
    return pl.ds(pl.multiple_of(index * width, width), width)


def span_kernel(
    table_in,
    q_in,
    pk_in,
    pv_in,
    ck_in,
    cv_in,
    out,
    kv0,
    kv1,
    kv2,
    kv3,
    qs,
    own,
    table,
    picked,
    acc,
    stat,
    ans,
    ahead_sem,
    back_sem,
    twin_sem,
    link_sem,
    twin_recv,
    side_sem,
    load_sem,
    q_send,
    q_recv,
    own_send,
    pass_send,
    own_recv,
    table_send,
    table_recv,
    picked_sem,
    ans_send,
    ans_recv,
):
    kv = (kv0, kv1, kv2, kv3)
    me, r = lax.axis_index("ctx"), lax.axis_index("rep")
    z, y = me // 2, me % 2
    side = z // 2
    inner = (z + side) % 2
    z_twin = z + 1 - 2 * (z % 2)
    z_ahead = inner * (3 - z) + (1 - inner) * z_twin
    is_inner, is_outer = inner == 1, inner == 0
    group = q_in.shape[2] // pk_in.shape[2]
    width = group * HEAD_WIDTH
    blocks_here = ck_in.shape[0]
    half = blocks_here // 2
    count = q_in.shape[0]

    def remote(src, dst, send, recv, ctx, rep):
        return pltpu.make_async_remote_copy(
            src_ref=src,
            dst_ref=dst,
            send_sem=send,
            recv_sem=recv,
            device_id={"ctx": ctx, "rep": rep},
            device_id_type=MESH,
        )

    def chunk_at(j):
        jj = j // 2
        m = jj + inner * (1 - 2 * jj) * (1 - jj // 2)
        return (m + side * (3 - 2 * m)) * 2 + (y + j % 2) % 2

    def lane(p, ctx, rep):
        return kv[p].at[pl.ds(ctx * blocks_here + rep * half, half)]

    barrier = pltpu.get_barrier_semaphore()

    def greet(ctx, rep):
        pl.semaphore_signal(barrier, inc=1, device_id={"ctx": ctx, "rep": rep}, device_id_type=MESH)

    beside = z * 2 + 1 - y
    greet(me, 1 - r)
    greet(beside, r)
    greet(z_twin * 2 + y, r)
    greet(z_twin * 2 + 1 - y, r)

    loads = []
    for p in range(PHASES):
        cols = aligned(2 * y + p // 2, HEAD_WIDTH)
        for kind, source in enumerate((ck_in, cv_in)):
            loads.append(
                pltpu.make_async_copy(
                    source.at[:, p % 2, :, cols],
                    kv[p].at[pl.ds(me * blocks_here, blocks_here), kind],
                    load_sem.at[p, kind],
                )
            )
    for load in loads:
        load.start()

    @pl.when(is_inner)
    def _():
        greet((3 - z) * 2 + y, r)
        pl.semaphore_wait(barrier, 5)

    @pl.when(is_outer)
    def _():
        pl.semaphore_wait(barrier, 4)

    def side_copies(p):
        cols = aligned(2 * (1 - y) + p // 2, HEAD_WIDTH)
        return [
            remote(
                source.at[pl.ds(r * half, half), p % 2, :, cols],
                kv[p].at[pl.ds(me * blocks_here + r * half, half), kind],
                side_sem.at[p, kind],
                link_sem.at[p, me],
                beside,
                r,
            )
            for kind, source in enumerate((ck_in, cv_in))
        ]

    def feeds():
        todo = []

        def add(cond, grp, other, ctx, slot):
            head = 2 * (1 - y if other else y) + grp
            place = 2 * grp + slot
            near = slot == 0
            items = [
                (
                    q_in.at[:, :, aligned(head, width)],
                    qs.at[place],
                    q_send.at[2 * grp + other],
                    q_recv.at[place],
                )
            ]
            for kind, source in enumerate((pk_in, pv_in)):
                items.append(
                    (
                        source.at[:, :, aligned(head, HEAD_WIDTH)],
                        own.at[place, kind, r],
                        own_send.at[4 * grp + 2 * other + kind],
                        own_recv.at[place, kind, r],
                    )
                )
            for src, dst, send, recv in items:
                if near:
                    todo.append((cond, pltpu.make_async_copy(src, dst, recv), True, (grp, other)))
                else:
                    copy = remote(src, dst, send, recv, ctx, r)
                    todo.append((cond, copy, False, (grp, other)))

        add(None, 0, 0, me, 0)
        add(None, 0, 1, beside, 1)
        add(is_inner, 1, 0, me, 0)
        add(is_inner, 1, 1, beside, 1)
        add(is_outer, 1, 0, z_twin * 2 + y, 2)
        add(is_outer, 1, 1, z_twin * 2 + 1 - y, 3)
        return todo

    def pass_own(place):
        return [
            remote(
                own.at[place, kind, 0],
                own.at[place, kind, 0],
                pass_send.at[place, kind],
                own_recv.at[place, kind, 0],
                me,
                1,
            )
            for kind in range(2)
        ]

    def table_copies():
        return [
            (None, remote(table_in, table.at[1], table_send.at[0], table_recv.at[1], beside, r)),
            (
                is_outer,
                remote(
                    table_in, table.at[2], table_send.at[1], table_recv.at[2], z_twin * 2 + y, r
                ),
            ),
            (
                is_outer,
                remote(
                    table_in, table.at[3], table_send.at[2], table_recv.at[3], z_twin * 2 + 1 - y, r
                ),
            ),
        ]

    def guarded(cond, action):
        if cond is None:
            action()
        else:
            pl.when(cond)(action)

    def ahead_copy(p, j):
        ctx = chunk_at(j)
        return remote(
            lane(p, ctx, r), lane(p, ctx, r), ahead_sem.at[p, j], link_sem.at[p, ctx],
            z_ahead * 2 + y, r,
        )

    def back_copy(p, j):
        ctx = chunk_at(j)
        return remote(
            lane(p, ctx, r), lane(p, ctx, r), back_sem.at[p, j], link_sem.at[p, ctx],
            z_twin * 2 + y, r,
        )

    def twin_copy(p, j):
        ctx = chunk_at(j)
        return remote(
            lane(p, ctx, r), lane(p, ctx, r), twin_sem.at[p, j], twin_recv.at[p, ctx], me, 1 - r
        )

    def goes(p, j):
        found = [(j < 2 + 2 * inner, ahead_copy(p, j))]
        if p < 2:
            found.append((is_inner & ((j < 2) | (j >= 4)), back_copy(p, j)))
        return found

    def relay(p, j, hold=False):
        ctx = chunk_at(j)
        ref = lane(p, ctx, r)
        remote(ref, ref, twin_sem.at[p, j], link_sem.at[p, ctx], me, 1 - r).wait_recv()
        for cond, copy in goes(p, j)[1 if hold else 0 :]:
            guarded(cond, copy.start)
        guarded(None if p < 2 else is_inner, twin_copy(p, j).start)

    def push(p, j):
        cond, copy = goes(p, j)[0]
        guarded(cond, copy.start)

    def load(p):
        loads[2 * p].wait()
        loads[2 * p + 1].wait()

    def complete(p):
        def one(j, carry):
            ctx = chunk_at(j)
            remote(
                lane(p, ctx, 1 - r), lane(p, ctx, 1 - r), twin_sem.at[p, j], twin_recv.at[p, ctx],
                me, 1 - r,
            ).wait_recv()
            return carry

        lax.fori_loop(1, CHUNKS, one, 0)

    todo = feeds()

    def feed(grp, other):
        for item in todo:
            if not item[2] and item[3] == (grp, other):
                guarded(item[0], item[1].start)

    for item in todo:
        if item[2]:
            guarded(item[0], item[1].start)
    for copy in side_copies(0):
        copy.start()
    for cond, copy in table_copies():
        guarded(cond, copy.start)
    load(0)
    push(0, 0)
    for copy in side_copies(1):
        copy.start()
    load(1)
    push(1, 0)
    feed(0, 1)
    load(2)
    load(3)

    @pl.when(is_inner)
    def _():
        back_copy(0, 0).start()
        back_copy(1, 0).start()

    for copy in side_copies(2) + side_copies(3):
        copy.start()

    @pl.when(is_inner)
    def _():
        feed(1, 1)

    def await_slot(place):
        pltpu.make_async_copy(qs.at[place], qs.at[place], q_recv.at[place]).wait()
        for kind in range(2):
            ref = own.at[place, kind, r]
            pltpu.make_async_copy(ref, ref, own_recv.at[place, kind, r]).wait()

        @pl.when(r == 0)
        def _():
            for copy in pass_own(place):
                copy.start()

        @pl.when(r == 1)
        def _():
            for kind in range(2):
                ref = own.at[place, kind, 0]
                pltpu.make_async_copy(ref, ref, own_recv.at[place, kind, 0]).wait()

    def query(t, u):
        return qs[t // count, t % count, :, u * HEAD_WIDTH : (u + 1) * HEAD_WIDTH]

    def own_unit(t):
        place, b = t // count, t % count

        def attend(earlier):
            row = lax.broadcasted_iota(jnp.int32, (ROWS, ROWS), 0)
            column = lax.broadcasted_iota(jnp.int32, (ROWS, ROWS), 1)
            for u in range(group):
                parts = [jnp.where(column <= row, score(query(t, u), own[place, 0, r, b]), NEGATIVE)]
                values = [own[place, 1, r, b]]
                if earlier:
                    parts.append(score(query(t, u), own[place, 0, 0, b]))
                    values.append(own[place, 1, 0, b])
                stat[t, u], acc[t, u] = fold(parts, values, None, None)

        pl.when(r == 0)(lambda: attend(False))
        pl.when(r == 1)(lambda: attend(True))

    def pick_unit(p, t):
        place, b = t // count, t % count
        grp, last = p // 2, p % 2 == 1
        slot = place - 2 * grp
        head = (2 * y + grp) * group
        for u in range(group):
            first = picked[slot, 0, b, head + u]
            second = picked[slot, 1, b, head + u]
            rows = query(t, u)
            peak, mixed = fold(
                [score(rows, kv[p][first, 0]), score(rows, kv[p][second, 0])],
                [kv[p][first, 1], kv[p][second, 1]],
                stat[t, u],
                acc[t, u],
            )
            if last:
                share = mixed[:, :HEAD_WIDTH] / mixed[:, HEAD_WIDTH:]
                ans[t, :, u * HEAD_WIDTH : (u + 1) * HEAD_WIDTH] = share.astype(ans.dtype)
            else:
                stat[t, u] = peak
                acc[t, u] = mixed

    def answer(t, grp, act_near, act_far):
        place, b = t // count, t % count
        slot = place - 2 * grp
        head = 2 * y + grp
        target = out.at[b, :, aligned(head, width)]
        zt = z + (slot // 2) * (z_twin - z)
        ctx = zt * 2 + (y + slot % 2) % 2

        @pl.when(slot == 0)
        def _():
            act_near(pltpu.make_async_copy(ans.at[t], target, ans_send.at[t]))

        @pl.when(slot > 0)
        def _():
            act_far(
                remote(ans.at[t], target, ans_send.at[t], ans_recv.at[head * count + b], ctx, r)
            )

    def send_answer(grp, t):
        answer(t, grp, lambda c: c.start(), lambda c: c.start())

    def stage(first, units, unit, relays, after=None):
        def one(i, carry):
            unit(first + i)
            if after is not None:
                pl.when(i > 0)(lambda: after(first + i - 1))
            for k, act in enumerate(relays):
                pl.when(i == (k + 1) * units // len(relays) - 1)(act)
            return carry

        lax.fori_loop(0, units, one, 0)

    def chain(*steps):
        def act():
            for step in steps:
                step()

        return act

    def at(p, j, hold=False):
        return lambda: relay(p, j, hold)

    def own_slot(place, *relays):
        await_slot(place)
        stage(place * count, count, own_unit, relays)

    def picks(p, slot, slots, *relays):
        grp, last = p // 2, p % 2 == 1
        first, units = (2 * grp + slot) * count, slots * count
        after = functools.partial(send_answer, grp) if last else None
        stage(first, units, functools.partial(pick_unit, p), relays, after)
        if last:
            send_answer(grp, first + units - 1)

    pltpu.make_async_copy(table_in, table.at[0], table_recv.at[0]).start()

    def await_table(slots):
        for slot in range(slots):
            pltpu.make_async_copy(table.at[slot], table.at[slot], table_recv.at[slot]).wait()
        copy = pltpu.make_async_copy(
            table.at[pl.ds(0, slots)], picked.at[pl.ds(0, slots)], picked_sem.at[0]
        )
        copy.start()
        copy.wait()

    @pl.when(is_inner)
    def _():
        own_slot(0, at(0, 1))
        own_slot(2, at(0, 2), at(0, 3))
        for p, j in ((0, 4), (1, 1), (1, 2), (1, 4), (0, 5), (1, 3), (0, 6)):
            relay(p, j)
        push(2, 0)
        relay(0, 7)
        await_table(4)
        own_slot(1)
        complete(0)
        picks(0, 0, 2, at(1, 5), at(2, 1), at(2, 2), at(1, 6))
        push(3, 0)
        relay(1, 7)
        complete(1)
        picks(1, 1, 1, at(3, 1, True))
        picks(1, 0, 1, at(2, 4))
        own_slot(4, at(2, 3), chain(lambda: push(3, 1), at(3, 2)))
        own_slot(3, at(2, 5), at(3, 3))
        relay(2, 6)
        relay(2, 7)
        complete(2)
        picks(2, 0, 3, at(3, 4))
        own_slot(5, at(3, 5))
        picks(2, 3, 1, at(3, 6))
        relay(3, 7)
        complete(3)
        picks(3, 2, 2)
        picks(3, 1, 1)
        picks(3, 0, 1)

    @pl.when(is_outer)
    def _():
        own_slot(0, at(0, 1))
        relay(1, 1)
        push(2, 0)
        push(3, 0)
        feed(1, 0)
        await_table(2)
        own_slot(1)
        relay(2, 1)
        relay(3, 1)
        feed(1, 1)
        lax.fori_loop(2, CHUNKS, lambda j, c: (relay(0, j), c)[1], 0)
        complete(0)
        picks(0, 0, 2, *[at(1, j) for j in range(2, 5)])
        lax.fori_loop(5, CHUNKS, lambda j, c: (relay(1, j), c)[1], 0)
        complete(1)
        picks(1, 1, 1)
        picks(1, 0, 1)

    for item in todo:
        if not item[2]:
            guarded(item[0], item[1].wait_send)
    for cond, copy in table_copies():
        guarded(cond, copy.wait_send)
    for p in range(PHASES):
        for copy in side_copies(p):
            copy.wait_send()

        def drain(j, carry):
            for cond, copy in goes(p, j):
                guarded(cond, copy.wait_send)
            twin = j >= 1 if p < 2 else (j >= 1) & is_inner
            guarded(twin, twin_copy(p, j).wait_send)
            return carry

        lax.fori_loop(0, CHUNKS, drain, 0)

    for place in range(6):
        sent = r == 0 if place < 2 else (r == 0) & is_inner

        @pl.when(sent)
        def _():
            for copy in pass_own(place):
                copy.wait_send()

    def settle(grp, t, carry):
        answer(t, grp, lambda c: c.wait(), lambda c: c.wait_send())
        return carry

    lax.fori_loop(0, 2 * count, functools.partial(settle, 0), 0)

    @pl.when(is_inner)
    def _():
        lax.fori_loop(2 * count, 6 * count, functools.partial(settle, 1), 0)

    def landed(k, carry):
        head, b = k // count, k % count
        target = out.at[b, :, aligned(head, width)]
        near = (head // 2 == y) & ((head % 2 == 0) | is_inner)

        @pl.when(jnp.logical_not(near))
        def _():
            remote(target, target, ans_send.at[0], ans_recv.at[k], me, 1 - r).wait_recv()

        return carry

    lax.fori_loop(0, 4 * count, landed, 0)


def spread_body(queries, prefill_keys, prefill_values, context_keys, context_values, picks):
    count, height, full = queries.shape
    key_heads = prefill_keys.shape[2] // HEAD_WIDTH
    group = full // prefill_keys.shape[2]
    blocks_here = context_keys.shape[0] // BLOCK_TOKENS
    blocks = blocks_here * CHUNKS
    units = 6 * count
    table = jnp.transpose(picks, (2, 0, 1))
    split = (blocks_here, 2, ROWS, context_keys.shape[1])
    dma = pltpu.SemaphoreType.DMA
    anywhere = pl.BlockSpec(memory_space=pl.ANY)
    work = (2 * LINE + 4 * 4) * count * group * key_heads // 4
    return pl.pallas_call(
        span_kernel,
        out_shape=jax.ShapeDtypeStruct(queries.shape, queries.dtype),
        in_specs=[anywhere] * 6,
        out_specs=anywhere,
        scratch_shapes=[pltpu.VMEM((blocks, 2, ROWS, HEAD_WIDTH), jnp.bfloat16)] * PHASES
        + [
            pltpu.VMEM((6, count, height, group * HEAD_WIDTH), jnp.bfloat16),
            pltpu.VMEM((6, 2, 2, count, height, HEAD_WIDTH), jnp.bfloat16),
            pltpu.VMEM((4,) + table.shape, jnp.int32),
            pltpu.SMEM((4,) + table.shape, jnp.int32),
            pltpu.VMEM((units, group, height, 2 * HEAD_WIDTH), jnp.float32),
            pltpu.VMEM((units, group, height, HEAD_WIDTH), jnp.float32),
            pltpu.VMEM((units, height, group * HEAD_WIDTH), jnp.bfloat16),
            dma((PHASES, CHUNKS)),
            dma((PHASES, CHUNKS)),
            dma((PHASES, CHUNKS)),
            dma((PHASES, CHUNKS)),
            dma((PHASES, CHUNKS)),
            dma((PHASES, 2)),
            dma((PHASES, 2)),
            dma((4,)),
            dma((6,)),
            dma((8,)),
            dma((6, 2)),
            dma((6, 2, 2)),
            dma((3,)),
            dma((4,)),
            dma((1,)),
            dma((units,)),
            dma((4 * count,)),
        ],
        compiler_params=pltpu.CompilerParams(
            collective_id=0, has_side_effects=True, vmem_limit_bytes=50 * 2**20
        ),
        cost_estimate=pl.CostEstimate(
            flops=work * 4 * ROWS * BLOCK_TOKENS * HEAD_WIDTH,
            transcendentals=work * ROWS * BLOCK_TOKENS,
            bytes_accessed=24 * 2**20,
        ),
        name="spread_attend",
    )(
        *[
            pltpu.with_memory_space_constraint(x, pltpu.HBM)
            for x in (
                table,
                queries,
                prefill_keys,
                prefill_values,
                context_keys.reshape(split),
                context_values.reshape(split),
            )
        ]
    )


def body(*args):
    queries, prefill_keys, _, context_keys, _, _ = args
    key_heads = prefill_keys.shape[2] // HEAD_WIDTH
    fits = lax.axis_size("ctx") == CHUNKS and lax.axis_size("rep") == 2 and key_heads == 4
    fits = fits and queries.shape[1] == ROWS and context_keys.shape[0] % (2 * BLOCK_TOKENS) == 0
    if fits:
        return spread_body(*args)
    return routed_body(*args)


def solution(mesh):
    return jax.shard_map(
        body,
        mesh=mesh,
        in_specs=(
            P(("groups", "ctx"), "rep", "head"),
            P(("groups", "ctx"), "rep", "head"),
            P(("groups", "ctx"), "rep", "head"),
            P(("groups", "ctx"), "head"),
            P(("groups", "ctx"), "head"),
            P(("groups", "ctx"), "head", None),
        ),
        out_specs=P(("groups", "ctx"), "rep", "head"),
        check_vma=False,
    )
```

```python
import functools
import math

import jax
import jax.numpy as jnp
from jax import lax
from jax.experimental import pallas as pl
from jax.experimental.pallas import tpu as pltpu
from jax.sharding import PartitionSpec as P


HEAD_WIDTH = 128
BLOCK_TOKENS = 512


NEGATIVE = -1e30


def from_behind(value, axis, steps):
    count = lax.axis_size(axis)
    first, last = (max(0, -steps), min(count, count - steps))
    return lax.ppermute(value, axis, [(source, source + steps) for source in range(first, last)])


def partial_attention(scores, values, allowed, pattern):
    scores = jnp.where(allowed, scores, NEGATIVE)
    highest = jnp.max(scores, axis=-1, keepdims=True)
    weights = jnp.exp(scores - highest)
    totals = jnp.sum(weights, axis=-1, keepdims=True)
    mixed = jnp.einsum(
        pattern, weights.astype(jnp.bfloat16), values, preferred_element_type=jnp.float32
    )
    return (mixed / totals, highest[..., 0] + jnp.log(totals[..., 0]))


def assign_slots(chosen, blocks_here, capacity):
    flat = chosen.reshape(-1)
    holders = flat // blocks_here
    places = jnp.arange(flat.shape[0])
    earlier = jnp.sum(
        (holders[:, None] == holders[None, :]) & (places[None, :] < places[:, None]), axis=1
    )
    return (holders * capacity + earlier, flat - holders * blocks_here)


def routed_body(queries, prefill_keys, prefill_values, context_keys, context_values, picks):
    local_count = queries.shape[0]
    stack_height = queries.shape[1]
    query_heads = queries.shape[2] // HEAD_WIDTH
    key_heads = prefill_keys.shape[2] // HEAD_WIDTH
    head_grouping = query_heads // key_heads
    blocks_here = context_keys.shape[0] // BLOCK_TOKENS
    ctx_size = lax.axis_size("ctx")
    pick_count = 2 * local_count * query_heads
    capacity = max(2, 2 * pick_count // ctx_size)
    slot_count = ctx_size * capacity
    scale = HEAD_WIDTH ** (-0.5)
    rep_index = lax.axis_index("rep")
    earlier_keys, earlier_values = from_behind((prefill_keys, prefill_values), "rep", 1)
    selected_block_keys = jnp.concatenate([earlier_keys, prefill_keys], 1).reshape(
        local_count, 2 * stack_height, key_heads, HEAD_WIDTH
    )
    selected_block_values = jnp.concatenate([earlier_values, prefill_values], 1).reshape(
        local_count, 2 * stack_height, key_heads, HEAD_WIDTH
    )
    grouped = queries.reshape(local_count, stack_height, key_heads, head_grouping, HEAD_WIDTH)
    query_place = rep_index * stack_height + jnp.arange(stack_height)
    key_place = (rep_index - 1) * stack_height + jnp.arange(2 * stack_height)
    allowed = (key_place[None, :] <= query_place[:, None]) & (key_place[None, :] >= 0)

    def own_block(paired):
        rows_here, keys_here, values_here = paired
        scores = (
            jnp.einsum("rkgd,jkd->kgrj", rows_here, keys_here, preferred_element_type=jnp.float32)
            * scale
        )
        return partial_attention(scores, values_here, allowed, "kgrj,jkd->kgrd")

    own_mixed, own_log = lax.map(own_block, (grouped, selected_block_keys, selected_block_values))
    own_mixed = own_mixed.reshape(local_count, query_heads, stack_height, HEAD_WIDTH)
    own_log = own_log.reshape(local_count, query_heads, stack_height)
    targets, local_blocks = assign_slots(picks[:, :, :2], blocks_here, capacity)
    routing = targets[:, None] == jnp.arange(slot_count)[None, :]
    sending = routing.astype(jnp.bfloat16).reshape(local_count, query_heads, 2, slot_count)
    by_head = queries.reshape(local_count, stack_height, query_heads, HEAD_WIDTH)
    outbound = jnp.einsum("qhps,qrhd->srd", sending, by_head, preferred_element_type=jnp.float32)
    outbound = outbound.astype(jnp.bfloat16).reshape(ctx_size, capacity, stack_height, HEAD_WIDTH)
    pick_heads = jnp.arange(pick_count) // 2 % query_heads // head_grouping
    key_tiles = context_keys.reshape(blocks_here, BLOCK_TOKENS, key_heads, HEAD_WIDTH)
    value_tiles = context_values.reshape(blocks_here, BLOCK_TOKENS, key_heads, HEAD_WIDTH)
    block_label = jnp.sum(jnp.where(routing, local_blocks[:, None], 0), axis=0)
    head_label = jnp.sum(jnp.where(routing, pick_heads[:, None], 0), axis=0)
    labels = jnp.stack([block_label, head_label], axis=-1).reshape(ctx_size, capacity, 2)
    inbound = lax.all_to_all(outbound, "ctx", split_axis=0, concat_axis=0, tiled=True)
    arrived = lax.all_to_all(labels, "ctx", split_axis=0, concat_axis=0, tiled=True)
    leading = inbound.shape[:2]

    def single(paired):
        rows_in, position = paired
        anchor = (position[0], 0, position[1], 0)
        keys_tile = lax.dynamic_slice(key_tiles, anchor, (1, BLOCK_TOKENS, 1, HEAD_WIDTH)).reshape(
            BLOCK_TOKENS, HEAD_WIDTH
        )
        values_tile = lax.dynamic_slice(
            value_tiles, anchor, (1, BLOCK_TOKENS, 1, HEAD_WIDTH)
        ).reshape(BLOCK_TOKENS, HEAD_WIDTH)
        scores = (
            lax.dot_general(
                rows_in, keys_tile, (((1,), (1,)), ((), ())), preferred_element_type=jnp.float32
            )
            * scale
        )
        mixed, logged = partial_attention(scores, values_tile, True, "rj,jd->rd")
        return (mixed.astype(jnp.bfloat16), logged)

    flat_rows = inbound.reshape((-1,) + inbound.shape[2:])
    flat_labels = arrived.reshape(-1, 2)
    mixed, logged = lax.map(single, (flat_rows, flat_labels), batch_size=8)
    served = mixed.reshape(leading + mixed.shape[1:])
    served_logs = logged.reshape(leading + logged.shape[1:])
    answers = lax.all_to_all(served, "ctx", split_axis=0, concat_axis=0, tiled=True)
    answer_logs = lax.all_to_all(served_logs, "ctx", split_axis=0, concat_axis=0, tiled=True)
    gathered = answers.reshape(slot_count, stack_height, HEAD_WIDTH)[targets]
    gathered_logs = answer_logs.reshape(slot_count, stack_height)[targets]
    remote_mixed = gathered.astype(jnp.float32).reshape(
        local_count, query_heads, 2, stack_height, HEAD_WIDTH
    )
    remote_logs = gathered_logs.reshape(local_count, query_heads, 2, stack_height)
    all_logs = jnp.concatenate([own_log[:, :, None], remote_logs], axis=2)
    all_mixed = jnp.concatenate([own_mixed[:, :, None], remote_mixed], axis=2)
    peak = jnp.max(all_logs, axis=2, keepdims=True)
    shares = jnp.exp(all_logs - peak)
    merged = jnp.sum(shares[..., None] * all_mixed, axis=2) / jnp.sum(shares, axis=2)[..., None]
    return (
        jnp.transpose(merged, (0, 2, 1, 3))
        .reshape(local_count, stack_height, query_heads * HEAD_WIDTH)
        .astype(jnp.bfloat16)
    )


RATE = HEAD_WIDTH ** (-0.5) * math.log2(math.e)
MESH = pl.DeviceIdType.MESH
LINE = 4
ROWS = BLOCK_TOKENS // 2
PHASES = 4
CHUNKS = 2 * LINE


def score(rows, keys):
    return lax.dot_general(
        rows, keys, (((1,), (1,)), ((), ())), preferred_element_type=jnp.float32
    )


def fold(parts, values, peak, mixed):
    highest = None
    for part in parts:
        for at in range(0, part.shape[1], HEAD_WIDTH):
            piece = part[:, at : at + HEAD_WIDTH]
            highest = piece if highest is None else jnp.maximum(highest, piece)
    highest = jnp.max(highest, axis=-1, keepdims=True)
    highest = jnp.broadcast_to(highest, (parts[0].shape[0], HEAD_WIDTH))
    if peak is not None:
        highest = jnp.maximum(peak, highest)
        fade = jnp.exp2((peak - highest) * RATE)
        mixed = mixed * jnp.concatenate([fade, fade], axis=1)
    level = highest * RATE
    for part, value in zip(parts, values):
        base = jnp.concatenate([level] * (part.shape[1] // HEAD_WIDTH), axis=1)
        weights = jnp.exp2(part * RATE - base).astype(jnp.bfloat16)
        beside = jnp.concatenate([value, jnp.ones_like(value)], axis=1)
        product = jnp.dot(weights, beside, preferred_element_type=jnp.float32)
        mixed = product if mixed is None else mixed + product
    return highest, mixed


def aligned(index, width):
    return pl.ds(pl.multiple_of(index * width, width), width)


def span_kernel(
    table_in,
    q_in,
    pk_in,
    pv_in,
    ck_in,
    cv_in,
    out,
    kv0,
    kv1,
    kv2,
    kv3,
    qs,
    own,
    table,
    picked,
    acc,
    stat,
    ans,
    ahead_sem,
    back_sem,
    twin_sem,
    link_sem,
    twin_recv,
    side_sem,
    load_sem,
    q_send,
    q_recv,
    own_send,
    pass_send,
    own_recv,
    table_send,
    table_recv,
    picked_sem,
    ans_send,
    ans_recv,
):
    kv = (kv0, kv1, kv2, kv3)
    me, r = lax.axis_index("ctx"), lax.axis_index("rep")
    z, y = me // 2, me % 2
    side = z // 2
    inner = (z + side) % 2
    z_twin = z + 1 - 2 * (z % 2)
    z_ahead = inner * (3 - z) + (1 - inner) * z_twin
    is_inner, is_outer = inner == 1, inner == 0
    group = q_in.shape[2] // pk_in.shape[2]
    width = group * HEAD_WIDTH
    blocks_here = ck_in.shape[0]
    half = blocks_here // 2
    count = q_in.shape[0]

    def remote(src, dst, send, recv, ctx, rep):
        return pltpu.make_async_remote_copy(
            src_ref=src,
            dst_ref=dst,
            send_sem=send,
            recv_sem=recv,
            device_id={"ctx": ctx, "rep": rep},
            device_id_type=MESH,
        )

    def chunk_at(j):
        jj = j // 2
        m = jj + inner * (1 - 2 * jj) * (1 - jj // 2)
        return (m + side * (3 - 2 * m)) * 2 + (y + j % 2) % 2

    def lane(p, ctx, rep):
        return kv[p].at[pl.ds(ctx * blocks_here + rep * half, half)]

    loads = []
    for p in range(PHASES):
        cols = aligned(2 * y + p // 2, HEAD_WIDTH)
        for kind, source in enumerate((ck_in, cv_in)):
            loads.append(
                pltpu.make_async_copy(
                    source.at[:, p % 2, :, cols],
                    kv[p].at[pl.ds(me * blocks_here, blocks_here), kind],
                    load_sem.at[p, kind],
                )
            )
    for load in loads[:2]:
        load.start()

    barrier = pltpu.get_barrier_semaphore()

    def greet(ctx, rep):
        pl.semaphore_signal(barrier, inc=1, device_id={"ctx": ctx, "rep": rep}, device_id_type=MESH)

    beside = z * 2 + 1 - y
    greet(me, 1 - r)
    greet(beside, r)
    greet(z_twin * 2 + y, r)
    greet(z_twin * 2 + 1 - y, r)

    @pl.when(is_inner)
    def _():
        greet((3 - z) * 2 + y, r)
        pl.semaphore_wait(barrier, 5)

    @pl.when(is_outer)
    def _():
        pl.semaphore_wait(barrier, 4)

    def side_copies(p):
        cols = aligned(2 * (1 - y) + p // 2, HEAD_WIDTH)
        return [
            remote(
                source.at[pl.ds(r * half, half), p % 2, :, cols],
                kv[p].at[pl.ds(me * blocks_here + r * half, half), kind],
                side_sem.at[p, kind],
                link_sem.at[p, me],
                beside,
                r,
            )
            for kind, source in enumerate((ck_in, cv_in))
        ]

    def feeds():
        todo = []

        def add(cond, grp, other, ctx, slot):
            head = 2 * (1 - y if other else y) + grp
            place = 2 * grp + slot
            near = slot == 0
            items = [
                (
                    q_in.at[:, :, aligned(head, width)],
                    qs.at[place],
                    q_send.at[2 * grp + other],
                    q_recv.at[place],
                )
            ]
            for kind, source in enumerate((pk_in, pv_in)):
                items.append(
                    (
                        source.at[:, :, aligned(head, HEAD_WIDTH)],
                        own.at[place, kind, r],
                        own_send.at[4 * grp + 2 * other + kind],
                        own_recv.at[place, kind, r],
                    )
                )
            for src, dst, send, recv in items:
                if near:
                    todo.append((cond, pltpu.make_async_copy(src, dst, recv), True, (grp, other)))
                else:
                    copy = remote(src, dst, send, recv, ctx, r)
                    todo.append((cond, copy, False, (grp, other)))

        add(None, 0, 0, me, 0)
        add(None, 0, 1, beside, 1)
        add(is_inner, 1, 0, me, 0)
        add(is_inner, 1, 1, beside, 1)
        add(is_outer, 1, 0, z_twin * 2 + y, 2)
        add(is_outer, 1, 1, z_twin * 2 + 1 - y, 3)
        return todo

    def pass_own(place):
        return [
            remote(
                own.at[place, kind, 0],
                own.at[place, kind, 0],
                pass_send.at[place, kind],
                own_recv.at[place, kind, 0],
                me,
                1,
            )
            for kind in range(2)
        ]

    def table_copies():
        return [
            (None, remote(table_in, table.at[1], table_send.at[0], table_recv.at[1], beside, r)),
            (
                is_outer,
                remote(
                    table_in, table.at[2], table_send.at[1], table_recv.at[2], z_twin * 2 + y, r
                ),
            ),
            (
                is_outer,
                remote(
                    table_in, table.at[3], table_send.at[2], table_recv.at[3], z_twin * 2 + 1 - y, r
                ),
            ),
        ]

    def guarded(cond, action):
        if cond is None:
            action()
        else:
            pl.when(cond)(action)

    def ahead_copy(p, j):
        ctx = chunk_at(j)
        return remote(
            lane(p, ctx, r), lane(p, ctx, r), ahead_sem.at[p, j], link_sem.at[p, ctx],
            z_ahead * 2 + y, r,
        )

    def back_copy(p, j):
        ctx = chunk_at(j)
        return remote(
            lane(p, ctx, r), lane(p, ctx, r), back_sem.at[p, j], link_sem.at[p, ctx],
            z_twin * 2 + y, r,
        )

    def twin_copy(p, j):
        ctx = chunk_at(j)
        return remote(
            lane(p, ctx, r), lane(p, ctx, r), twin_sem.at[p, j], twin_recv.at[p, ctx], me, 1 - r
        )

    def goes(p, j):
        found = [(j < 2 + 2 * inner, ahead_copy(p, j))]
        if p < 2:
            found.append((is_inner & ((j < 2) | (j >= 4)), back_copy(p, j)))
        return found

    def relay(p, j, hold=False):
        ctx = chunk_at(j)
        ref = lane(p, ctx, r)
        remote(ref, ref, twin_sem.at[p, j], link_sem.at[p, ctx], me, 1 - r).wait_recv()
        for cond, copy in goes(p, j)[1 if hold else 0 :]:
            guarded(cond, copy.start)
        guarded(None if p < 2 else is_inner, twin_copy(p, j).start)

    def push(p, j):
        cond, copy = goes(p, j)[0]
        guarded(cond, copy.start)

    def load(p):
        loads[2 * p].wait()
        loads[2 * p + 1].wait()

    def complete(p):
        def one(j, carry):
            ctx = chunk_at(j)
            remote(
                lane(p, ctx, 1 - r), lane(p, ctx, 1 - r), twin_sem.at[p, j], twin_recv.at[p, ctx],
                me, 1 - r,
            ).wait_recv()
            return carry

        lax.fori_loop(1, CHUNKS, one, 0)

    todo = feeds()

    def feed(grp, other):
        for item in todo:
            if not item[2] and item[3] == (grp, other):
                guarded(item[0], item[1].start)

    load(0)
    push(0, 0)
    for copy in side_copies(0):
        copy.start()
    for copy in loads[2:]:
        copy.start()
    for item in todo:
        if item[2]:
            guarded(item[0], item[1].start)
    for cond, copy in table_copies():
        guarded(cond, copy.start)
    for copy in side_copies(1):
        copy.start()
    load(1)
    push(1, 0)
    feed(0, 1)
    load(2)
    load(3)

    @pl.when(is_inner)
    def _():
        back_copy(0, 0).start()
        back_copy(1, 0).start()

    for copy in side_copies(2) + side_copies(3):
        copy.start()

    @pl.when(is_inner)
    def _():
        feed(1, 1)

    def await_slot(place):
        pltpu.make_async_copy(qs.at[place], qs.at[place], q_recv.at[place]).wait()
        for kind in range(2):
            ref = own.at[place, kind, r]
            pltpu.make_async_copy(ref, ref, own_recv.at[place, kind, r]).wait()

        @pl.when(r == 0)
        def _():
            for copy in pass_own(place):
                copy.start()

        @pl.when(r == 1)
        def _():
            for kind in range(2):
                ref = own.at[place, kind, 0]
                pltpu.make_async_copy(ref, ref, own_recv.at[place, kind, 0]).wait()

    def query(t, u):
        return qs[t // count, t % count, :, u * HEAD_WIDTH : (u + 1) * HEAD_WIDTH]

    def own_unit(t):
        place, b = t // count, t % count

        def attend(earlier):
            row = lax.broadcasted_iota(jnp.int32, (ROWS, ROWS), 0)
            column = lax.broadcasted_iota(jnp.int32, (ROWS, ROWS), 1)
            for u in range(group):
                parts = [jnp.where(column <= row, score(query(t, u), own[place, 0, r, b]), NEGATIVE)]
                values = [own[place, 1, r, b]]
                if earlier:
                    parts.append(score(query(t, u), own[place, 0, 0, b]))
                    values.append(own[place, 1, 0, b])
                stat[t, u], acc[t, u] = fold(parts, values, None, None)

        pl.when(r == 0)(lambda: attend(False))
        pl.when(r == 1)(lambda: attend(True))

    def pick_unit(p, t):
        place, b = t // count, t % count
        grp, last = p // 2, p % 2 == 1
        slot = place - 2 * grp
        head = (2 * y + grp) * group
        for u in range(group):
            first = picked[slot, 0, b, head + u]
            second = picked[slot, 1, b, head + u]
            rows = query(t, u)
            peak, mixed = fold(
                [score(rows, kv[p][first, 0]), score(rows, kv[p][second, 0])],
                [kv[p][first, 1], kv[p][second, 1]],
                stat[t, u],
                acc[t, u],
            )
            if last:
                share = mixed[:, :HEAD_WIDTH] / mixed[:, HEAD_WIDTH:]
                ans[t, :, u * HEAD_WIDTH : (u + 1) * HEAD_WIDTH] = share.astype(ans.dtype)
            else:
                stat[t, u] = peak
                acc[t, u] = mixed

    def answer(t, grp, act_near, act_far):
        place, b = t // count, t % count
        slot = place - 2 * grp
        head = 2 * y + grp
        target = out.at[b, :, aligned(head, width)]
        zt = z + (slot // 2) * (z_twin - z)
        ctx = zt * 2 + (y + slot % 2) % 2

        @pl.when(slot == 0)
        def _():
            act_near(pltpu.make_async_copy(ans.at[t], target, ans_send.at[t]))

        @pl.when(slot > 0)
        def _():
            act_far(
                remote(ans.at[t], target, ans_send.at[t], ans_recv.at[head * count + b], ctx, r)
            )

    def send_answer(grp, t):
        answer(t, grp, lambda c: c.start(), lambda c: c.start())

    def stage(first, units, unit, relays, after=None):
        def one(i, carry):
            unit(first + i)
            if after is not None:
                after(first + i)
            for k, act in enumerate(relays):
                pl.when(i == (k + 1) * units // len(relays) - 1)(act)
            return carry

        lax.fori_loop(0, units, one, 0)

    def chain(*steps):
        def act():
            for step in steps:
                step()

        return act

    def at(p, j, hold=False):
        return lambda: relay(p, j, hold)

    def own_slot(place, *relays):
        await_slot(place)
        stage(place * count, count, own_unit, relays)

    def picks(p, slot, slots, *relays):
        grp, last = p // 2, p % 2 == 1
        first, units = (2 * grp + slot) * count, slots * count
        after = functools.partial(send_answer, grp) if last else None
        stage(first, units, functools.partial(pick_unit, p), relays, after)

    pltpu.make_async_copy(table_in, table.at[0], table_recv.at[0]).start()

    def await_table(slots):
        for slot in range(slots):
            pltpu.make_async_copy(table.at[slot], table.at[slot], table_recv.at[slot]).wait()
        copy = pltpu.make_async_copy(
            table.at[pl.ds(0, slots)], picked.at[pl.ds(0, slots)], picked_sem.at[0]
        )
        copy.start()
        copy.wait()

    @pl.when(is_inner)
    def _():
        own_slot(0, at(0, 1))
        own_slot(2, at(0, 2), at(0, 3))
        for p, j in ((0, 4), (1, 1), (1, 2), (1, 4), (0, 5), (1, 3), (0, 6)):
            relay(p, j)
        push(2, 0)
        relay(0, 7)
        await_table(4)
        own_slot(1)
        complete(0)
        picks(0, 0, 2, at(1, 5), at(2, 1), at(2, 2), at(1, 6))
        push(3, 0)
        relay(1, 7)
        complete(1)
        picks(1, 1, 1, at(3, 1, True))
        picks(1, 0, 1, at(2, 4))
        own_slot(4, at(2, 3), chain(lambda: push(3, 1), at(3, 2)))
        own_slot(3, at(2, 5), at(3, 3))
        relay(2, 6)
        relay(2, 7)
        complete(2)
        picks(2, 0, 3, at(3, 4))
        own_slot(5, at(3, 5))
        picks(2, 3, 1, at(3, 6))
        relay(3, 7)
        complete(3)
        picks(3, 3, 1)
        picks(3, 2, 1)
        picks(3, 1, 1)
        picks(3, 0, 1)

    @pl.when(is_outer)
    def _():
        own_slot(0, at(0, 1))
        relay(1, 1)
        push(2, 0)
        push(3, 0)
        feed(1, 0)
        await_table(2)
        own_slot(1)
        relay(2, 1)
        relay(3, 1)
        feed(1, 1)
        lax.fori_loop(2, CHUNKS, lambda j, c: (relay(0, j), c)[1], 0)
        complete(0)
        picks(0, 0, 2, *[at(1, j) for j in range(2, 5)])
        lax.fori_loop(5, CHUNKS, lambda j, c: (relay(1, j), c)[1], 0)
        complete(1)
        picks(1, 1, 1)
        picks(1, 0, 1)

    for item in todo:
        if not item[2]:
            guarded(item[0], item[1].wait_send)
    for cond, copy in table_copies():
        guarded(cond, copy.wait_send)
    for p in range(PHASES):
        for copy in side_copies(p):
            copy.wait_send()

        def drain(j, carry):
            for cond, copy in goes(p, j):
                guarded(cond, copy.wait_send)
            twin = j >= 1 if p < 2 else (j >= 1) & is_inner
            guarded(twin, twin_copy(p, j).wait_send)
            return carry

        lax.fori_loop(0, CHUNKS, drain, 0)

    for place in range(6):
        sent = r == 0 if place < 2 else (r == 0) & is_inner

        @pl.when(sent)
        def _():
            for copy in pass_own(place):
                copy.wait_send()

    def settle(grp, t, carry):
        answer(t, grp, lambda c: c.wait(), lambda c: c.wait_send())
        return carry

    lax.fori_loop(0, 2 * count, functools.partial(settle, 0), 0)

    @pl.when(is_inner)
    def _():
        lax.fori_loop(2 * count, 6 * count, functools.partial(settle, 1), 0)

    def landed(k, carry):
        head, b = k // count, k % count
        target = out.at[b, :, aligned(head, width)]
        near = (head // 2 == y) & ((head % 2 == 0) | is_inner)

        @pl.when(jnp.logical_not(near))
        def _():
            remote(target, target, ans_send.at[0], ans_recv.at[k], me, 1 - r).wait_recv()

        return carry

    lax.fori_loop(0, 4 * count, landed, 0)


def spread_body(queries, prefill_keys, prefill_values, context_keys, context_values, picks):
    count, height, full = queries.shape
    key_heads = prefill_keys.shape[2] // HEAD_WIDTH
    group = full // prefill_keys.shape[2]
    blocks_here = context_keys.shape[0] // BLOCK_TOKENS
    blocks = blocks_here * CHUNKS
    units = 6 * count
    table = jnp.transpose(picks, (2, 0, 1))
    split = (blocks_here, 2, ROWS, context_keys.shape[1])
    dma = pltpu.SemaphoreType.DMA
    anywhere = pl.BlockSpec(memory_space=pl.ANY)
    work = (2 * LINE + 4 * 4) * count * group * key_heads // 4
    return pl.pallas_call(
        span_kernel,
        out_shape=jax.ShapeDtypeStruct(queries.shape, queries.dtype),
        in_specs=[anywhere] * 6,
        out_specs=anywhere,
        scratch_shapes=[pltpu.VMEM((blocks, 2, ROWS, HEAD_WIDTH), jnp.bfloat16)] * PHASES
        + [
            pltpu.VMEM((6, count, height, group * HEAD_WIDTH), jnp.bfloat16),
            pltpu.VMEM((6, 2, 2, count, height, HEAD_WIDTH), jnp.bfloat16),
            pltpu.VMEM((4,) + table.shape, jnp.int32),
            pltpu.SMEM((4,) + table.shape, jnp.int32),
            pltpu.VMEM((units, group, height, 2 * HEAD_WIDTH), jnp.float32),
            pltpu.VMEM((units, group, height, HEAD_WIDTH), jnp.float32),
            pltpu.VMEM((units, height, group * HEAD_WIDTH), jnp.bfloat16),
            dma((PHASES, CHUNKS)),
            dma((PHASES, CHUNKS)),
            dma((PHASES, CHUNKS)),
            dma((PHASES, CHUNKS)),
            dma((PHASES, CHUNKS)),
            dma((PHASES, 2)),
            dma((PHASES, 2)),
            dma((4,)),
            dma((6,)),
            dma((8,)),
            dma((6, 2)),
            dma((6, 2, 2)),
            dma((3,)),
            dma((4,)),
            dma((1,)),
            dma((units,)),
            dma((4 * count,)),
        ],
        compiler_params=pltpu.CompilerParams(
            collective_id=0, has_side_effects=True, vmem_limit_bytes=50 * 2**20
        ),
        cost_estimate=pl.CostEstimate(
            flops=work * 4 * ROWS * BLOCK_TOKENS * HEAD_WIDTH,
            transcendentals=work * ROWS * BLOCK_TOKENS,
            bytes_accessed=24 * 2**20,
        ),
        name="spread_attend",
    )(
        *[
            pltpu.with_memory_space_constraint(x, pltpu.HBM)
            for x in (
                table,
                queries,
                prefill_keys,
                prefill_values,
                context_keys.reshape(split),
                context_values.reshape(split),
            )
        ]
    )


def body(*args):
    queries, prefill_keys, _, context_keys, _, _ = args
    key_heads = prefill_keys.shape[2] // HEAD_WIDTH
    fits = lax.axis_size("ctx") == CHUNKS and lax.axis_size("rep") == 2 and key_heads == 4
    fits = fits and queries.shape[1] == ROWS and context_keys.shape[0] % (2 * BLOCK_TOKENS) == 0
    if fits:
        return spread_body(*args)
    return routed_body(*args)


def solution(mesh):
    return jax.shard_map(
        body,
        mesh=mesh,
        in_specs=(
            P(("groups", "ctx"), "rep", "head"),
            P(("groups", "ctx"), "rep", "head"),
            P(("groups", "ctx"), "rep", "head"),
            P(("groups", "ctx"), "head"),
            P(("groups", "ctx"), "head"),
            P(("groups", "ctx"), "head", None),
        ),
        out_specs=P(("groups", "ctx"), "rep", "head"),
        check_vma=False,
    )
```

```python
import functools
import math

import jax
import jax.numpy as jnp
from jax import lax
from jax.experimental import pallas as pl
from jax.experimental.pallas import tpu as pltpu
from jax.sharding import PartitionSpec as P


HEAD_WIDTH = 128
BLOCK_TOKENS = 512


NEGATIVE = -1e30


def from_behind(value, axis, steps):
    count = lax.axis_size(axis)
    first, last = (max(0, -steps), min(count, count - steps))
    return lax.ppermute(value, axis, [(source, source + steps) for source in range(first, last)])


def partial_attention(scores, values, allowed, pattern):
    scores = jnp.where(allowed, scores, NEGATIVE)
    highest = jnp.max(scores, axis=-1, keepdims=True)
    weights = jnp.exp(scores - highest)
    totals = jnp.sum(weights, axis=-1, keepdims=True)
    mixed = jnp.einsum(
        pattern, weights.astype(jnp.bfloat16), values, preferred_element_type=jnp.float32
    )
    return (mixed / totals, highest[..., 0] + jnp.log(totals[..., 0]))


def assign_slots(chosen, blocks_here, capacity):
    flat = chosen.reshape(-1)
    holders = flat // blocks_here
    places = jnp.arange(flat.shape[0])
    earlier = jnp.sum(
        (holders[:, None] == holders[None, :]) & (places[None, :] < places[:, None]), axis=1
    )
    return (holders * capacity + earlier, flat - holders * blocks_here)


def routed_body(queries, prefill_keys, prefill_values, context_keys, context_values, picks):
    local_count = queries.shape[0]
    stack_height = queries.shape[1]
    query_heads = queries.shape[2] // HEAD_WIDTH
    key_heads = prefill_keys.shape[2] // HEAD_WIDTH
    head_grouping = query_heads // key_heads
    blocks_here = context_keys.shape[0] // BLOCK_TOKENS
    ctx_size = lax.axis_size("ctx")
    pick_count = 2 * local_count * query_heads
    capacity = max(2, 2 * pick_count // ctx_size)
    slot_count = ctx_size * capacity
    scale = HEAD_WIDTH ** (-0.5)
    rep_index = lax.axis_index("rep")
    earlier_keys, earlier_values = from_behind((prefill_keys, prefill_values), "rep", 1)
    selected_block_keys = jnp.concatenate([earlier_keys, prefill_keys], 1).reshape(
        local_count, 2 * stack_height, key_heads, HEAD_WIDTH
    )
    selected_block_values = jnp.concatenate([earlier_values, prefill_values], 1).reshape(
        local_count, 2 * stack_height, key_heads, HEAD_WIDTH
    )
    grouped = queries.reshape(local_count, stack_height, key_heads, head_grouping, HEAD_WIDTH)
    query_place = rep_index * stack_height + jnp.arange(stack_height)
    key_place = (rep_index - 1) * stack_height + jnp.arange(2 * stack_height)
    allowed = (key_place[None, :] <= query_place[:, None]) & (key_place[None, :] >= 0)

    def own_block(paired):
        rows_here, keys_here, values_here = paired
        scores = (
            jnp.einsum("rkgd,jkd->kgrj", rows_here, keys_here, preferred_element_type=jnp.float32)
            * scale
        )
        return partial_attention(scores, values_here, allowed, "kgrj,jkd->kgrd")

    own_mixed, own_log = lax.map(own_block, (grouped, selected_block_keys, selected_block_values))
    own_mixed = own_mixed.reshape(local_count, query_heads, stack_height, HEAD_WIDTH)
    own_log = own_log.reshape(local_count, query_heads, stack_height)
    targets, local_blocks = assign_slots(picks[:, :, :2], blocks_here, capacity)
    routing = targets[:, None] == jnp.arange(slot_count)[None, :]
    sending = routing.astype(jnp.bfloat16).reshape(local_count, query_heads, 2, slot_count)
    by_head = queries.reshape(local_count, stack_height, query_heads, HEAD_WIDTH)
    outbound = jnp.einsum("qhps,qrhd->srd", sending, by_head, preferred_element_type=jnp.float32)
    outbound = outbound.astype(jnp.bfloat16).reshape(ctx_size, capacity, stack_height, HEAD_WIDTH)
    pick_heads = jnp.arange(pick_count) // 2 % query_heads // head_grouping
    key_tiles = context_keys.reshape(blocks_here, BLOCK_TOKENS, key_heads, HEAD_WIDTH)
    value_tiles = context_values.reshape(blocks_here, BLOCK_TOKENS, key_heads, HEAD_WIDTH)
    block_label = jnp.sum(jnp.where(routing, local_blocks[:, None], 0), axis=0)
    head_label = jnp.sum(jnp.where(routing, pick_heads[:, None], 0), axis=0)
    labels = jnp.stack([block_label, head_label], axis=-1).reshape(ctx_size, capacity, 2)
    inbound = lax.all_to_all(outbound, "ctx", split_axis=0, concat_axis=0, tiled=True)
    arrived = lax.all_to_all(labels, "ctx", split_axis=0, concat_axis=0, tiled=True)
    leading = inbound.shape[:2]

    def single(paired):
        rows_in, position = paired
        anchor = (position[0], 0, position[1], 0)
        keys_tile = lax.dynamic_slice(key_tiles, anchor, (1, BLOCK_TOKENS, 1, HEAD_WIDTH)).reshape(
            BLOCK_TOKENS, HEAD_WIDTH
        )
        values_tile = lax.dynamic_slice(
            value_tiles, anchor, (1, BLOCK_TOKENS, 1, HEAD_WIDTH)
        ).reshape(BLOCK_TOKENS, HEAD_WIDTH)
        scores = (
            lax.dot_general(
                rows_in, keys_tile, (((1,), (1,)), ((), ())), preferred_element_type=jnp.float32
            )
            * scale
        )
        mixed, logged = partial_attention(scores, values_tile, True, "rj,jd->rd")
        return (mixed.astype(jnp.bfloat16), logged)

    flat_rows = inbound.reshape((-1,) + inbound.shape[2:])
    flat_labels = arrived.reshape(-1, 2)
    mixed, logged = lax.map(single, (flat_rows, flat_labels), batch_size=8)
    served = mixed.reshape(leading + mixed.shape[1:])
    served_logs = logged.reshape(leading + logged.shape[1:])
    answers = lax.all_to_all(served, "ctx", split_axis=0, concat_axis=0, tiled=True)
    answer_logs = lax.all_to_all(served_logs, "ctx", split_axis=0, concat_axis=0, tiled=True)
    gathered = answers.reshape(slot_count, stack_height, HEAD_WIDTH)[targets]
    gathered_logs = answer_logs.reshape(slot_count, stack_height)[targets]
    remote_mixed = gathered.astype(jnp.float32).reshape(
        local_count, query_heads, 2, stack_height, HEAD_WIDTH
    )
    remote_logs = gathered_logs.reshape(local_count, query_heads, 2, stack_height)
    all_logs = jnp.concatenate([own_log[:, :, None], remote_logs], axis=2)
    all_mixed = jnp.concatenate([own_mixed[:, :, None], remote_mixed], axis=2)
    peak = jnp.max(all_logs, axis=2, keepdims=True)
    shares = jnp.exp(all_logs - peak)
    merged = jnp.sum(shares[..., None] * all_mixed, axis=2) / jnp.sum(shares, axis=2)[..., None]
    return (
        jnp.transpose(merged, (0, 2, 1, 3))
        .reshape(local_count, stack_height, query_heads * HEAD_WIDTH)
        .astype(jnp.bfloat16)
    )


RATE = HEAD_WIDTH ** (-0.5) * math.log2(math.e)
MESH = pl.DeviceIdType.MESH
LINE = 4
ROWS = BLOCK_TOKENS // 2
PHASES = 4
CHUNKS = 2 * LINE


def score(rows, keys):
    return lax.dot_general(
        rows, keys, (((1,), (1,)), ((), ())), preferred_element_type=jnp.float32
    )


def fold(parts, values, peak, mixed):
    highest = None
    for part in parts:
        for at in range(0, part.shape[1], HEAD_WIDTH):
            piece = part[:, at : at + HEAD_WIDTH]
            highest = piece if highest is None else jnp.maximum(highest, piece)
    highest = jnp.max(highest, axis=-1, keepdims=True)
    highest = jnp.broadcast_to(highest, (parts[0].shape[0], HEAD_WIDTH))
    if peak is not None:
        highest = jnp.maximum(peak, highest)
        fade = jnp.exp2((peak - highest) * RATE)
        mixed = mixed * jnp.concatenate([fade, fade], axis=1)
    level = highest * RATE
    for part, value in zip(parts, values):
        base = jnp.concatenate([level] * (part.shape[1] // HEAD_WIDTH), axis=1)
        weights = jnp.exp2(part * RATE - base).astype(jnp.bfloat16)
        beside = jnp.concatenate([value, jnp.ones_like(value)], axis=1)
        product = jnp.dot(weights, beside, preferred_element_type=jnp.float32)
        mixed = product if mixed is None else mixed + product
    return highest, mixed


def aligned(index, width):
    return pl.ds(pl.multiple_of(index * width, width), width)


def span_kernel(
    table_in,
    q_in,
    pk_in,
    pv_in,
    ck_in,
    cv_in,
    out,
    kv0,
    kv1,
    kv2,
    kv3,
    qs,
    own,
    table,
    picked,
    acc,
    stat,
    ans,
    ahead_sem,
    back_sem,
    twin_sem,
    link_sem,
    twin_recv,
    side_sem,
    load_sem,
    q_send,
    q_recv,
    own_send,
    pass_send,
    own_recv,
    table_send,
    table_recv,
    picked_sem,
    ans_send,
    ans_recv,
):
    kv = (kv0, kv1, kv2, kv3)
    me, r = lax.axis_index("ctx"), lax.axis_index("rep")
    z, y = me // 2, me % 2
    side = z // 2
    inner = (z + side) % 2
    z_twin = z + 1 - 2 * (z % 2)
    z_ahead = inner * (3 - z) + (1 - inner) * z_twin
    is_inner, is_outer = inner == 1, inner == 0
    group = q_in.shape[2] // pk_in.shape[2]
    width = group * HEAD_WIDTH
    blocks_here = ck_in.shape[0]
    half = blocks_here // 2
    count = q_in.shape[0]

    def remote(src, dst, send, recv, ctx, rep):
        return pltpu.make_async_remote_copy(
            src_ref=src,
            dst_ref=dst,
            send_sem=send,
            recv_sem=recv,
            device_id={"ctx": ctx, "rep": rep},
            device_id_type=MESH,
        )

    def chunk_at(j):
        jj = j // 2
        m = jj + inner * (1 - 2 * jj) * (1 - jj // 2)
        return (m + side * (3 - 2 * m)) * 2 + (y + j % 2) % 2

    def lane(p, ctx, rep):
        return kv[p].at[pl.ds(ctx * blocks_here + rep * half, half)]

    loads = []
    for p in range(PHASES):
        cols = aligned(2 * y + p // 2, HEAD_WIDTH)
        for kind, source in enumerate((ck_in, cv_in)):
            loads.append(
                pltpu.make_async_copy(
                    source.at[:, p % 2, :, cols],
                    kv[p].at[pl.ds(me * blocks_here, blocks_here), kind],
                    load_sem.at[p, kind],
                )
            )
    for load in loads[:2]:
        load.start()

    barrier = pltpu.get_barrier_semaphore()

    def greet(ctx, rep):
        pl.semaphore_signal(barrier, inc=1, device_id={"ctx": ctx, "rep": rep}, device_id_type=MESH)

    beside = z * 2 + 1 - y
    greet(me, 1 - r)
    greet(beside, r)
    greet(z_twin * 2 + y, r)
    greet(z_twin * 2 + 1 - y, r)

    @pl.when(is_inner)
    def _():
        greet((3 - z) * 2 + y, r)
        pl.semaphore_wait(barrier, 5)

    @pl.when(is_outer)
    def _():
        pl.semaphore_wait(barrier, 4)

    def side_copies(p):
        cols = aligned(2 * (1 - y) + p // 2, HEAD_WIDTH)
        return [
            remote(
                source.at[pl.ds(r * half, half), p % 2, :, cols],
                kv[p].at[pl.ds(me * blocks_here + r * half, half), kind],
                side_sem.at[p, kind],
                link_sem.at[p, me],
                beside,
                r,
            )
            for kind, source in enumerate((ck_in, cv_in))
        ]

    def feeds():
        todo = []

        def add(cond, grp, other, ctx, slot):
            head = 2 * (1 - y if other else y) + grp
            place = 2 * grp + slot
            near = slot == 0
            items = [
                (
                    q_in.at[:, :, aligned(head, width)],
                    qs.at[place],
                    q_send.at[2 * grp + other],
                    q_recv.at[place],
                )
            ]
            for kind, source in enumerate((pk_in, pv_in)):
                items.append(
                    (
                        source.at[:, :, aligned(head, HEAD_WIDTH)],
                        own.at[place, kind, r],
                        own_send.at[4 * grp + 2 * other + kind],
                        own_recv.at[place, kind, r],
                    )
                )
            for src, dst, send, recv in items:
                if near:
                    todo.append((cond, pltpu.make_async_copy(src, dst, recv), True, (grp, other)))
                else:
                    copy = remote(src, dst, send, recv, ctx, r)
                    todo.append((cond, copy, False, (grp, other)))

        add(None, 0, 0, me, 0)
        add(None, 0, 1, beside, 1)
        add(is_inner, 1, 0, me, 0)
        add(is_inner, 1, 1, beside, 1)
        add(is_outer, 1, 0, z_twin * 2 + y, 2)
        add(is_outer, 1, 1, z_twin * 2 + 1 - y, 3)
        return todo

    def pass_own(place):
        return [
            remote(
                own.at[place, kind, 0],
                own.at[place, kind, 0],
                pass_send.at[place, kind],
                own_recv.at[place, kind, 0],
                me,
                1,
            )
            for kind in range(2)
        ]

    def table_copies():
        return [
            (None, remote(table_in, table.at[1], table_send.at[0], table_recv.at[1], beside, r)),
            (
                is_outer,
                remote(
                    table_in, table.at[2], table_send.at[1], table_recv.at[2], z_twin * 2 + y, r
                ),
            ),
            (
                is_outer,
                remote(
                    table_in, table.at[3], table_send.at[2], table_recv.at[3], z_twin * 2 + 1 - y, r
                ),
            ),
        ]

    def guarded(cond, action):
        if cond is None:
            action()
        else:
            pl.when(cond)(action)

    def ahead_copy(p, j):
        ctx = chunk_at(j)
        return remote(
            lane(p, ctx, r), lane(p, ctx, r), ahead_sem.at[p, j], link_sem.at[p, ctx],
            z_ahead * 2 + y, r,
        )

    def back_copy(p, j):
        ctx = chunk_at(j)
        return remote(
            lane(p, ctx, r), lane(p, ctx, r), back_sem.at[p, j], link_sem.at[p, ctx],
            z_twin * 2 + y, r,
        )

    def twin_copy(p, j):
        ctx = chunk_at(j)
        return remote(
            lane(p, ctx, r), lane(p, ctx, r), twin_sem.at[p, j], twin_recv.at[p, ctx], me, 1 - r
        )

    def goes(p, j):
        found = [(j < 2 + 2 * inner, ahead_copy(p, j))]
        if p < 2:
            found.append((is_inner & ((j < 2) | (j >= 4)), back_copy(p, j)))
        return found

    def relay(p, j, hold=False):
        ctx = chunk_at(j)
        ref = lane(p, ctx, r)
        remote(ref, ref, twin_sem.at[p, j], link_sem.at[p, ctx], me, 1 - r).wait_recv()
        for cond, copy in goes(p, j)[1 if hold else 0 :]:
            guarded(cond, copy.start)
        guarded(None if p < 2 else is_inner, twin_copy(p, j).start)

    def push(p, j):
        cond, copy = goes(p, j)[0]
        guarded(cond, copy.start)

    def load(p):
        loads[2 * p].wait()
        loads[2 * p + 1].wait()

    def complete(p, start=1, stop=CHUNKS):
        def one(j, carry):
            ctx = chunk_at(j)
            remote(
                lane(p, ctx, 1 - r), lane(p, ctx, 1 - r), twin_sem.at[p, j], twin_recv.at[p, ctx],
                me, 1 - r,
            ).wait_recv()
            return carry

        lax.fori_loop(start, stop, one, 0)

    todo = feeds()

    def feed(grp, other):
        for item in todo:
            if not item[2] and item[3] == (grp, other):
                guarded(item[0], item[1].start)

    load(0)
    push(0, 0)
    for copy in side_copies(0):
        copy.start()
    for copy in loads[2:]:
        copy.start()
    for item in todo:
        if item[2]:
            guarded(item[0], item[1].start)
    for cond, copy in table_copies():
        guarded(cond, copy.start)
    for copy in side_copies(1):
        copy.start()
    load(1)
    push(1, 0)
    feed(0, 1)
    load(2)
    load(3)

    @pl.when(is_inner)
    def _():
        back_copy(0, 0).start()
        back_copy(1, 0).start()

    for copy in side_copies(2) + side_copies(3):
        copy.start()

    @pl.when(is_inner)
    def _():
        feed(1, 1)

    def await_slot(place):
        pltpu.make_async_copy(qs.at[place], qs.at[place], q_recv.at[place]).wait()
        for kind in range(2):
            ref = own.at[place, kind, r]
            pltpu.make_async_copy(ref, ref, own_recv.at[place, kind, r]).wait()

        @pl.when(r == 0)
        def _():
            for copy in pass_own(place):
                copy.start()

        @pl.when(r == 1)
        def _():
            for kind in range(2):
                ref = own.at[place, kind, 0]
                pltpu.make_async_copy(ref, ref, own_recv.at[place, kind, 0]).wait()

    def query(t, u):
        return qs[t // count, t % count, :, u * HEAD_WIDTH : (u + 1) * HEAD_WIDTH]

    def own_unit(t):
        place, b = t // count, t % count

        def attend(earlier):
            row = lax.broadcasted_iota(jnp.int32, (ROWS, ROWS), 0)
            column = lax.broadcasted_iota(jnp.int32, (ROWS, ROWS), 1)
            for u in range(group):
                parts = [jnp.where(column <= row, score(query(t, u), own[place, 0, r, b]), NEGATIVE)]
                values = [own[place, 1, r, b]]
                if earlier:
                    parts.append(score(query(t, u), own[place, 0, 0, b]))
                    values.append(own[place, 1, 0, b])
                stat[t, u], acc[t, u] = fold(parts, values, None, None)

        pl.when(r == 0)(lambda: attend(False))
        pl.when(r == 1)(lambda: attend(True))

    def pick_unit(p, t, heads=range(group)):
        place, b = t // count, t % count
        grp, last = p // 2, p % 2 == 1
        slot = place - 2 * grp
        head = (2 * y + grp) * group
        for u in heads:
            first = picked[slot, 0, b, head + u]
            second = picked[slot, 1, b, head + u]
            rows = query(t, u)
            peak, mixed = fold(
                [score(rows, kv[p][first, 0]), score(rows, kv[p][second, 0])],
                [kv[p][first, 1], kv[p][second, 1]],
                stat[t, u],
                acc[t, u],
            )
            if last:
                share = mixed[:, :HEAD_WIDTH] / mixed[:, HEAD_WIDTH:]
                ans[t, :, u * HEAD_WIDTH : (u + 1) * HEAD_WIDTH] = share.astype(ans.dtype)
            else:
                stat[t, u] = peak
                acc[t, u] = mixed

    def answer(t, grp, act_near, act_far):
        place, b = t // count, t % count
        slot = place - 2 * grp
        head = 2 * y + grp
        target = out.at[b, :, aligned(head, width)]
        zt = z + (slot // 2) * (z_twin - z)
        ctx = zt * 2 + (y + slot % 2) % 2

        @pl.when(slot == 0)
        def _():
            act_near(pltpu.make_async_copy(ans.at[t], target, ans_send.at[t]))

        @pl.when(slot > 0)
        def _():
            act_far(
                remote(ans.at[t], target, ans_send.at[t], ans_recv.at[head * count + b], ctx, r)
            )

    def send_answer(grp, t):
        answer(t, grp, lambda c: c.start(), lambda c: c.start())

    def halves(t):
        b = t % count
        head = 2 * y + 1
        part = group // 2
        for side_at in range(2):
            pick_unit(3, t, range(side_at * part, (side_at + 1) * part))
            size = part * HEAD_WIDTH
            remote(
                ans.at[t, :, pl.ds(side_at * size, size)],
                out.at[b, :, aligned(head * 2 + side_at, size)],
                ans_send.at[t],
                ans_recv.at[head * count + b],
                z_twin * 2 + 1 - y,
                r,
            ).start()

    def stage(first, units, unit, relays, after=None):
        def one(i, carry):
            unit(first + i)
            if after is not None:
                after(first + i)
            for k, act in enumerate(relays):
                pl.when(i == (k + 1) * units // len(relays) - 1)(act)
            return carry

        lax.fori_loop(0, units, one, 0)

    def chain(*steps):
        def act():
            for step in steps:
                step()

        return act

    def at(p, j, hold=False):
        return lambda: relay(p, j, hold)

    def own_slot(place, *relays):
        await_slot(place)
        stage(place * count, count, own_unit, relays)

    def picks(p, slot, slots, *relays):
        grp, last = p // 2, p % 2 == 1
        first, units = (2 * grp + slot) * count, slots * count
        after = functools.partial(send_answer, grp) if last else None
        stage(first, units, functools.partial(pick_unit, p), relays, after)

    pltpu.make_async_copy(table_in, table.at[0], table_recv.at[0]).start()

    def await_table(slots):
        for slot in range(slots):
            pltpu.make_async_copy(table.at[slot], table.at[slot], table_recv.at[slot]).wait()
        copy = pltpu.make_async_copy(
            table.at[pl.ds(0, slots)], picked.at[pl.ds(0, slots)], picked_sem.at[0]
        )
        copy.start()
        copy.wait()

    @pl.when(is_inner)
    def _():
        own_slot(0, at(0, 1))
        own_slot(2, at(0, 2), at(0, 3))
        for p, j in ((0, 4), (1, 1), (1, 2), (1, 4), (0, 5), (1, 3), (0, 6)):
            relay(p, j)
        push(2, 0)
        relay(0, 7)
        await_table(4)
        own_slot(1)
        complete(0)
        picks(0, 0, 2, at(1, 5), at(2, 1), at(2, 2), at(1, 6))
        push(3, 0)
        relay(1, 7)
        complete(1)
        picks(1, 1, 1, at(3, 1, True))
        picks(1, 0, 1, at(2, 4))
        own_slot(4, at(2, 3), chain(lambda: push(3, 1), at(3, 2)))
        own_slot(3, at(2, 5), at(3, 3))
        relay(2, 6)
        relay(2, 7)
        complete(2)
        picks(2, 0, 3, at(3, 4))
        own_slot(5, at(3, 5))
        picks(2, 3, 1, at(3, 6))
        complete(3, 1, CHUNKS - 1)
        relay(3, 7)
        complete(3, CHUNKS - 1)
        stage(5 * count, count, halves, ())
        picks(3, 2, 1)
        picks(3, 1, 1)
        picks(3, 0, 1)

    @pl.when(is_outer)
    def _():
        own_slot(0, at(0, 1))
        relay(1, 1)
        push(2, 0)
        push(3, 0)
        feed(1, 0)
        await_table(2)
        own_slot(1)
        relay(2, 1)
        relay(3, 1)
        feed(1, 1)
        lax.fori_loop(2, CHUNKS, lambda j, c: (relay(0, j), c)[1], 0)
        complete(0)
        picks(0, 0, 2, *[at(1, j) for j in range(2, 5)])
        lax.fori_loop(5, CHUNKS, lambda j, c: (relay(1, j), c)[1], 0)
        complete(1)
        picks(1, 1, 1)
        picks(1, 0, 1)

    for item in todo:
        if not item[2]:
            guarded(item[0], item[1].wait_send)
    for cond, copy in table_copies():
        guarded(cond, copy.wait_send)
    for p in range(PHASES):
        for copy in side_copies(p):
            copy.wait_send()

        def drain(j, carry):
            for cond, copy in goes(p, j):
                guarded(cond, copy.wait_send)
            twin = j >= 1 if p < 2 else (j >= 1) & is_inner
            guarded(twin, twin_copy(p, j).wait_send)
            return carry

        lax.fori_loop(0, CHUNKS, drain, 0)

    for place in range(6):
        sent = r == 0 if place < 2 else (r == 0) & is_inner

        @pl.when(sent)
        def _():
            for copy in pass_own(place):
                copy.wait_send()

    def settle(grp, t, carry):
        answer(t, grp, lambda c: c.wait(), lambda c: c.wait_send())
        return carry

    lax.fori_loop(0, 2 * count, functools.partial(settle, 0), 0)

    @pl.when(is_inner)
    def _():
        lax.fori_loop(2 * count, 6 * count, functools.partial(settle, 1), 0)

    def landed(k, carry):
        head, b = k // count, k % count
        target = out.at[b, :, aligned(head, width)]
        near = (head // 2 == y) & ((head % 2 == 0) | is_inner)

        @pl.when(jnp.logical_not(near))
        def _():
            remote(target, target, ans_send.at[0], ans_recv.at[k], me, 1 - r).wait_recv()

        return carry

    lax.fori_loop(0, 4 * count, landed, 0)


def spread_body(queries, prefill_keys, prefill_values, context_keys, context_values, picks):
    count, height, full = queries.shape
    key_heads = prefill_keys.shape[2] // HEAD_WIDTH
    group = full // prefill_keys.shape[2]
    blocks_here = context_keys.shape[0] // BLOCK_TOKENS
    blocks = blocks_here * CHUNKS
    units = 6 * count
    table = jnp.transpose(picks, (2, 0, 1))
    split = (blocks_here, 2, ROWS, context_keys.shape[1])
    dma = pltpu.SemaphoreType.DMA
    anywhere = pl.BlockSpec(memory_space=pl.ANY)
    work = (2 * LINE + 4 * 4) * count * group * key_heads // 4
    return pl.pallas_call(
        span_kernel,
        out_shape=jax.ShapeDtypeStruct(queries.shape, queries.dtype),
        in_specs=[anywhere] * 6,
        out_specs=anywhere,
        scratch_shapes=[pltpu.VMEM((blocks, 2, ROWS, HEAD_WIDTH), jnp.bfloat16)] * PHASES
        + [
            pltpu.VMEM((6, count, height, group * HEAD_WIDTH), jnp.bfloat16),
            pltpu.VMEM((6, 2, 2, count, height, HEAD_WIDTH), jnp.bfloat16),
            pltpu.VMEM((4,) + table.shape, jnp.int32),
            pltpu.SMEM((4,) + table.shape, jnp.int32),
            pltpu.VMEM((units, group, height, 2 * HEAD_WIDTH), jnp.float32),
            pltpu.VMEM((units, group, height, HEAD_WIDTH), jnp.float32),
            pltpu.VMEM((units, height, group * HEAD_WIDTH), jnp.bfloat16),
            dma((PHASES, CHUNKS)),
            dma((PHASES, CHUNKS)),
            dma((PHASES, CHUNKS)),
            dma((PHASES, CHUNKS)),
            dma((PHASES, CHUNKS)),
            dma((PHASES, 2)),
            dma((PHASES, 2)),
            dma((4,)),
            dma((6,)),
            dma((8,)),
            dma((6, 2)),
            dma((6, 2, 2)),
            dma((3,)),
            dma((4,)),
            dma((1,)),
            dma((units,)),
            dma((4 * count,)),
        ],
        compiler_params=pltpu.CompilerParams(
            collective_id=0, has_side_effects=True, vmem_limit_bytes=50 * 2**20
        ),
        cost_estimate=pl.CostEstimate(
            flops=work * 4 * ROWS * BLOCK_TOKENS * HEAD_WIDTH,
            transcendentals=work * ROWS * BLOCK_TOKENS,
            bytes_accessed=24 * 2**20,
        ),
        name="spread_attend",
    )(
        *[
            pltpu.with_memory_space_constraint(x, pltpu.HBM)
            for x in (
                table,
                queries,
                prefill_keys,
                prefill_values,
                context_keys.reshape(split),
                context_values.reshape(split),
            )
        ]
    )


def body(*args):
    queries, prefill_keys, _, context_keys, _, _ = args
    key_heads = prefill_keys.shape[2] // HEAD_WIDTH
    fits = lax.axis_size("ctx") == CHUNKS and lax.axis_size("rep") == 2 and key_heads == 4
    fits = fits and queries.shape[1] == ROWS and context_keys.shape[0] % (2 * BLOCK_TOKENS) == 0
    if fits:
        return spread_body(*args)
    return routed_body(*args)


def solution(mesh):
    return jax.shard_map(
        body,
        mesh=mesh,
        in_specs=(
            P(("groups", "ctx"), "rep", "head"),
            P(("groups", "ctx"), "rep", "head"),
            P(("groups", "ctx"), "rep", "head"),
            P(("groups", "ctx"), "head"),
            P(("groups", "ctx"), "head"),
            P(("groups", "ctx"), "head", None),
        ),
        out_specs=P(("groups", "ctx"), "rep", "head"),
        check_vma=False,
    )
```
